32 devices in a mesh: gx: 8 (over z, y), gy: 4 (over x, core).
Axes of the slice: x: 2, y: 2, z: 4, core: 2. Of those that a mesh axis runs over, the one named last changes fastest.
Arguments:
- scalar: float32 [2, 512, 8, 4, 128], P(None, None, 'gx', 'gy'), may hold values from -6 to 6
- velocity: float32 [3, 2, 512, 8, 4, 128], P(None, None, None, 'gx', 'gy'), may hold values from -1 to 1
- diffusivity: float32 [2, 8, 4, 128], P(None, 'gx', 'gy'), may hold values from 0.005 to 0.05
- recv_owner: int32 [65536, 1], P(('gx', 'gy')), may hold values from 0 to 31; in each aligned block of 2048 rows (0 to 2047, 2048 to 4095, ...) at most 128 rows name the same one
- donor_elem: int32 [65536], P(('gx', 'gy')), may hold values from 0 to 127
- recv_point: int32 [65536], P(('gx', 'gy')), may hold values from 0 to 65535
- recv_coords: float32 [3, 65536], P(None, ('gx', 'gy')), may hold values from -1 to 1
Outputs:
- advanced: float32 [2, 512, 8, 4, 128], P(None, None, 'gx', 'gy')
The draws below stay inside these ranges and needn't reach their ends.
Inputs may be any that keep to these rules, and one draw needn't show every extreme that they name: `recv_owner`: among the 2048 receivers of one device no owner is named more than 128 times, a bound that some block reaches.
All inputs are finite; a program needn't handle non-finite values.
Results may differ from the reference program's by a relative error of at most 0.0003.
Values sent between devices are 32-bit elements; how exact they have to be, the bound alone decides.
A program may use at most 128 MiB of HBM per device.

```python
import math
import jax
import jax.numpy as jnp
import numpy as np
from jax import lax

KX = 1
KY = 1
EZ = 128
R_DEV = 2048
ELEMS = 128
CAP = 128
EX = 8
EY = 4
RECV = 65536
N_GY = 4
DEVICES = 32


def set_ends(entries, own_key, smallest, largest):
    spot = [jax.random.randint(jax.random.fold_in(own_key, axis), (), 0, length) for axis, length in enumerate(entries.shape)]
    main_axis = entries.shape.index(max(entries.shape))
    next_to = spot[:main_axis] + [(spot[main_axis] + 1) % entries.shape[main_axis]] + spot[main_axis + 1:]
    return entries.at[tuple(spot)].set(smallest).at[tuple(next_to)].set(largest)


def block_levels(own_key, extent, shards, smallest, top_value):
    def one(dim, parts):
        heights = jax.random.uniform(jax.random.fold_in(jax.random.fold_in(own_key, 6), dim), (parts,), jnp.float32, smallest / len(shards), top_value / len(shards))
        return jnp.repeat(jnp.exp(heights), extent[dim] // parts).reshape((-1,) + (1,) * (len(extent) - dim - 1))

    factor_of = one(*shards[0])
    for cut in shards[1:]:
        factor_of = factor_of * one(*cut)
    return factor_of


def routed_block(key, own, number, rows, amount, top, most, skew):
    order = jax.random.permutation(key, amount)
    crowded, usual = load_shares(amount, rows * top, most, skew, True), load_shares(amount, rows * top, most, skew, False)
    places = jnp.arange(amount)

    def named(sizes, offset_by):
        used = int((sizes > 0).sum())
        fixed = max(1, used // 4)
        passed = fixed + (places - fixed + offset_by * (used - fixed)) % max(1, amount - fixed)
        return jnp.zeros((amount,), jnp.int32).at[order[jnp.where(places < fixed, places, passed)]].set(jnp.asarray(sizes, jnp.int32))

    sizes = jnp.where(number % 4 == 0, named(crowded, number // 4), named(usual, number - number // 4 - 1))
    mixed = jax.random.permutation(jax.random.fold_in(own, 3), amount)
    source_of, sink = mixed[0:amount // 2 * 2:2], mixed[1:amount // 2 * 2:2]
    slack = jnp.minimum(sizes[source_of] - 1, most - sizes[sink]) // 2
    slack = jnp.where((source_of == order[0]) | (sink == order[0]) | (sizes[sink] == 0), 0, jnp.maximum(slack, 0))
    passed = jax.random.randint(jax.random.fold_in(own, 4), (amount // 2,), 0, 1 << 20) % (slack + 1)
    sizes = sizes.at[source_of].add(-passed).at[sink].add(passed)
    members = jnp.searchsorted(jnp.cumsum(sizes), jnp.arange(rows * top), side="right").astype(jnp.int32)
    grid = members.reshape(top, rows).T
    grid = grid[jax.random.permutation(jax.random.fold_in(own, 1), rows)]
    offset_by = jax.random.randint(jax.random.fold_in(own, 2), (rows, 1), 0, top)
    return jnp.take_along_axis(grid, (jnp.arange(top)[None, :] + offset_by) % top, axis=1)


def load_shares(number_of, total, reach, lean, full):
    portions = [(1 << 20) // math.isqrt(grade ** lean) + 1 for grade in range(1, number_of + 1)]
    largest = reach if full else min(reach, max(-(-total // number_of), total * portions[0] // sum(portions)))
    least = 1 if total - largest >= number_of - 1 else 0
    holding, rest = [largest] + [least] * (number_of - 1), total - largest - least * (number_of - 1)
    while rest > 0:
        movable = [i for i in range(1, number_of) if holding[i] < largest] or [i for i in range(1, number_of) if holding[i] < reach]
        pool, remaining = sum([portions[i] for i in movable]), rest
        for i in movable:
            addition = min(reach - holding[i], max(1, remaining * portions[i] // pool), rest)
            holding[i] = holding[i] + addition
            rest = rest - addition
    return np.array(holding)


def bell_draw(rng, extent, scale, bound, shards=(), kind=jnp.bfloat16):
    loudness = block_levels(rng, extent, shards, -0.22, 0.18) if shards else 1.0
    result = jax.random.normal(rng, extent, jnp.float32) * scale * loudness
    return jnp.minimum(jnp.maximum(result, -bound), bound).astype(kind)


def setup_inputs(seed: int = 0) -> dict:
    streams_of = jax.random.split(jax.random.key(seed), 8)
    scalar = bell_draw(streams_of[0], (2, 512, EX, EY, EZ), 1.0, 6.0, ((2, 8), (3, 4)), jnp.float32)
    velocity = jnp.clip(jax.random.uniform(streams_of[1], (3, 2, 512, EX, EY, EZ), jnp.float32, -1.0, 1.0) * block_levels(streams_of[1], (3, 2, 512, EX, EY, EZ), ((3, 8), (4, 4)), -0.4, 0.0), -1.0, 1.0)
    diffusivity = jnp.clip(jnp.exp(math.log(0.05) - 2.3025851 * jax.random.uniform(streams_of[2], (2, EX, EY, EZ), jnp.float32) ** block_levels(streams_of[2], (2, EX, EY, EZ), ((1, 8), (2, 4)), -0.2, 0.2)), 0.005, 0.05)
    recv_owner_keys = jax.random.split(jax.random.fold_in(streams_of[3], 1), RECV // R_DEV)
    recv_owner_turns = jax.random.permutation(jax.random.fold_in(streams_of[3], 3), RECV // R_DEV)
    recv_owner = jax.vmap(lambda own, number: routed_block(jax.random.fold_in(streams_of[3], 2), own, number, R_DEV, DEVICES, 1, CAP, 2))(recv_owner_keys, recv_owner_turns).reshape((RECV, 1))
    donor_elem = set_ends(jax.random.randint(streams_of[4], (RECV,), 0, ELEMS), jax.random.fold_in(streams_of[4], 1), 0, ELEMS - 1).astype(jnp.int32)
    recv_point = set_ends(jax.random.randint(streams_of[5], (RECV,), 0, 512 * ELEMS), jax.random.fold_in(streams_of[5], 1), 0, (512 * ELEMS) - 1).astype(jnp.int32)
    recv_coords = jnp.clip(jax.random.uniform(streams_of[6], (3, RECV), jnp.float32, -1.0, 1.0) * block_levels(streams_of[6], (3, RECV), ((1, 32),), -0.4, 0.0), -1.0, 1.0)
    return {"scalar": scalar, "velocity": velocity, "diffusivity": diffusivity, "recv_owner": recv_owner, "donor_elem": donor_elem, "recv_point": recv_point, "recv_coords": recv_coords}


time_step = 0.01
penalty_rate = 50.0
metric = 2.0
volume_factor = 0.125
node_inner = [0.871740148509606615337, 0.591700181433142302144, 0.209299217902478868769]


def legendre_seven(point):
    before, current = 1.0, point
    for order in range(1, 7):
        before, current = current, ((2 * order + 1) * point * current - order * before) / (order + 1)
    return current


def gll_tables():
    degree = 7
    gll_nodes = [-1.0, -node_inner[0], -node_inner[1], -node_inner[2], node_inner[2], node_inner[1], node_inner[0], 1.0]
    end_values = [legendre_seven(v) for v in gll_nodes]
    weights = [2.0 / (degree * (degree + 1) * v * v) for v in end_values]
    derivative = [[0.0] * 8 for _ in range(8)]
    for a in range(8):
        for b in range(8):
            if a != b:
                derivative[a][b] = end_values[a] / (end_values[b] * (gll_nodes[a] - gll_nodes[b]))
    derivative[0][0] = -degree * (degree + 1) / 4.0
    derivative[7][7] = degree * (degree + 1) / 4.0
    weight_row = jnp.asarray(weights, jnp.float32)
    cube_weights = weight_row[:, None, None] * weight_row[None, :, None] * weight_row[None, None, :]
    return gll_nodes, cube_weights, derivative


def lagrange_rows(position, gll_nodes):
    columns = []
    for j in range(8):
        factor = jnp.ones_like(position)
        for m in range(8):
            if m != j:
                factor = factor * ((position - gll_nodes[m]) / (gll_nodes[j] - gll_nodes[m]))
        columns.append(factor)
    return jnp.stack(columns, axis=-1)


def element_rate(values, velocity, diffusivity, derivative, cube_weights):
    highest = lax.Precision.HIGHEST
    grad_x = metric * jnp.einsum('ai,ijkxyz->ajkxyz', derivative, values, precision=highest)
    grad_y = metric * jnp.einsum('bj,ijkxyz->ibkxyz', derivative, values, precision=highest)
    grad_z = metric * jnp.einsum('ck,ijkxyz->ijcxyz', derivative, values, precision=highest)
    mass_local = volume_factor * cube_weights[:, :, :, None, None, None]
    advect = velocity[0] * grad_x + velocity[1] * grad_y + velocity[2] * grad_z
    scaled = (metric * mass_local) * diffusivity[None, None, None]
    diffuse = jnp.einsum('ai,ajkxyz->ijkxyz', derivative, scaled * grad_x, precision=highest)
    diffuse = diffuse + jnp.einsum('bj,ibkxyz->ijkxyz', derivative, scaled * grad_y, precision=highest)
    diffuse = diffuse + jnp.einsum('ck,ijcxyz->ijkxyz', derivative, scaled * grad_z, precision=highest)
    return -(mass_local * advect) - diffuse


def face_sum(values, pdim, edim, next_slab, prev_slab):
    left = lax.index_in_dim(values, 0, pdim, keepdims=True)
    right = lax.index_in_dim(values, 7, pdim, keepdims=True)
    count = values.shape[edim]
    after = jnp.concatenate([lax.slice_in_dim(left, 1, count, axis=edim), next_slab], axis=edim)
    before = jnp.concatenate([prev_slab, lax.slice_in_dim(right, 0, count - 1, axis=edim)], axis=edim)
    middle = lax.slice_in_dim(values, 1, 7, axis=pdim)
    return jnp.concatenate([left + before, middle, right + after], axis=pdim)


def assemble(values):
    for pdim, edim in ((1, 4), (2, 5), (3, 6)):
        slab = lax.index_in_dim(lax.index_in_dim(values, 0, pdim, keepdims=True), 0, edim, keepdims=True)
        zeros_slab = jnp.zeros_like(slab)
        values = face_sum(values, pdim, edim, zeros_slab, zeros_slab)
    return values


def reference(scalar, velocity, diffusivity, recv_owner, donor_elem, recv_point, recv_coords):
    gll_nodes, cube_np, derivative_np = gll_tables()
    derivative = jnp.asarray(derivative_np, jnp.float32)
    cube_weights = jnp.asarray(cube_np, jnp.float32)
    cube_flat = cube_weights.reshape(512)
    shape_full = (2, 8, 8, 8, EX, EY, EZ)
    elems = KX * KY * EZ
    flow = velocity.reshape((3,) + shape_full)
    mass_total = assemble(jnp.broadcast_to(volume_factor * cube_weights[None, :, :, :, None, None, None], shape_full))

    rows = jnp.arange(RECV, dtype=jnp.int32)
    device = rows // R_DEV
    local_row = rows % R_DEV
    dev_x = device // N_GY
    dev_y = device % N_GY
    own_mesh = (local_row >= R_DEV // 2).astype(jnp.int32)
    donor_mesh = 1 - own_mesh
    owners = recv_owner[:, 0]
    donor_x = (owners // N_GY) * KX + donor_elem // (KY * EZ)
    donor_y = (owners % N_GY) * KY + (donor_elem // EZ) % KY
    donor_z = donor_elem % EZ
    point_q = recv_point // elems
    point_e = recv_point % elems
    recv_x = dev_x * KX + point_e // (KY * EZ)
    recv_y = dev_y * KY + (point_e // EZ) % KY
    recv_z = point_e % EZ
    flat_index = ((own_mesh * 512 + point_q) * EX + recv_x) * (EY * EZ) + recv_y * EZ + recv_z
    basis_x = lagrange_rows(recv_coords[0], gll_nodes)
    basis_y = lagrange_rows(recv_coords[1], gll_nodes)
    basis_z = lagrange_rows(recv_coords[2], gll_nodes)
    point_mass = volume_factor * cube_flat[point_q]

    def blocks(array):
        return array.reshape((DEVICES, R_DEV) + array.shape[1:])

    def interpolate(values_five):
        def one_block(pieces):
            mesh_ids, elem_x, elem_y, elem_z, wx, wy, wz = pieces
            element_values = values_five[mesh_ids, :, elem_x, elem_y, elem_z]
            tensor_weights = (wx[:, :, None, None] * wy[:, None, :, None] * wz[:, None, None, :]).reshape(-1, 512)
            return jnp.sum(element_values * tensor_weights, axis=1)
        pieces = (blocks(donor_mesh), blocks(donor_x), blocks(donor_y), blocks(donor_z),
                  blocks(basis_x), blocks(basis_y), blocks(basis_z))
        return lax.map(one_block, pieces).reshape(RECV)

    def rate(values):
        local = jnp.stack([element_rate(values[m], flow[:, m], diffusivity[m], derivative, cube_weights) for m in range(2)])
        donor_values = interpolate(values.reshape(2, 512, EX, EY, EZ))
        current = values.reshape(-1)[flat_index]
        added = penalty_rate * point_mass * (donor_values - current)
        local = local.reshape(-1).at[flat_index].add(added).reshape(shape_full)
        return assemble(local) / mass_total

    start = scalar.reshape(shape_full)
    first = start + time_step * rate(start)
    second = 0.75 * start + 0.25 * (first + time_step * rate(first))
    third = start / 3.0 + (2.0 / 3.0) * (second + time_step * rate(second))
    return third.reshape(2, 512, EX, EY, EZ)
```

```python
import functools
import jax
import jax.numpy as jnp
import numpy as np
from jax import lax
from jax.experimental import pallas as pl
from jax.experimental.pallas import tpu as pltpu
from jax.sharding import PartitionSpec as P

time_step = 0.01
penalty_rate = 50.0
volume_factor = 0.125
node_inner = [0.8717401485096066, 0.5917001814331423, 0.20929921790247888]


def legendre_seven(point):
    before, current = (1.0, point)
    for order in range(1, 7):
        before, current = (
            current,
            ((2 * order + 1) * point * current - order * before) / (order + 1),
        )
    return current


def gll_tables():
    degree = 7
    gll_nodes = [-1.0] + [-v for v in node_inner] + node_inner[::-1] + [1.0]
    end_values = [legendre_seven(v) for v in gll_nodes]
    weights = [2.0 / (degree * (degree + 1) * v * v) for v in end_values]
    derivative = [[0.0] * 8 for _ in range(8)]
    for a in range(8):
        for b in range(8):
            if a != b:
                derivative[a][b] = end_values[a] / (end_values[b] * (gll_nodes[a] - gll_nodes[b]))
    derivative[0][0] = -degree * (degree + 1) / 4.0
    derivative[7][7] = degree * (degree + 1) / 4.0
    return (gll_nodes, weights, derivative)


MESH = pl.DeviceIdType.MESH
HEADINGS = [(-1, 0), (1, 0), (0, -1), (0, 1), (-1, -1), (-1, 1), (1, -1), (1, 1)]


def halves(value):
    high = value.astype(jnp.bfloat16)
    return high, (value - high.astype(jnp.float32)).astype(jnp.bfloat16)


def mm(a, b):
    return jnp.dot(a, b, preferred_element_type=jnp.float32)


def mm_t(a, b):
    return lax.dot_general(a, b, (((1,), (1,)), ((), ())), preferred_element_type=jnp.float32)


def mm3(op_high, op_low, value):
    high, low = halves(value)
    return mm(op_high, high) + mm(op_high, low) + mm(op_low, high)


def step_kernel(
    tables, owner_ref, elem_ref, point_ref, coord_ref, nu_ref, start_hbm, vel_hbm, ops_hbm,
    out_ref,
    start, vel, ops, cur, local, work, grad, wm, dim, held,
    hot_s, within_s, rank_s, asked, got, pick, basis_ref, spread_q, spread_e,
    ans, rep, hx, hy, he,
    in_sem, ask_send, ask_recv, ans_send, ans_recv, halo_send, halo_recv,
):
    gll_nodes, weights, derivative = tables
    f32, bf, i32 = jnp.float32, jnp.bfloat16, jnp.int32
    gx, gy = lax.axis_index("gx"), lax.axis_index("gy")
    nx, ny = lax.axis_size("gx"), lax.axis_size("gy")
    n = nx * ny
    me = gx * ny + gy
    ez = start.shape[-1]
    rows = owner_ref.shape[-1]
    cap = ans.shape[-1]
    groups, _, lanes = pick.shape
    per = lanes // cap
    width = within_s.shape[-1]
    blocks = rows // width
    half_rows = rows // 2

    barrier = pltpu.get_barrier_semaphore()

    def place(d):
        return (d // ny, lax.rem(d, ny))

    def greet(step, carry):
        d = lax.rem(me + step, n)
        pl.semaphore_signal(barrier, inc=1, device_id=place(d), device_id_type=MESH)
        return carry

    lax.fori_loop(1, n, greet, 0)
    loads = [
        pltpu.make_async_copy(start_hbm, start, in_sem.at[0]),
        pltpu.make_async_copy(vel_hbm, vel, in_sem.at[1]),
        pltpu.make_async_copy(ops_hbm, ops, in_sem.at[2]),
    ]
    for load in loads:
        load.start()

    for b in range(blocks):
        spot = slice(b * width, (b + 1) * width)
        iota_n = lax.broadcasted_iota(i32, (n, width), 0)
        hot_s[b * n:(b + 1) * n, :] = jnp.where(owner_ref[0:1, spot] == iota_n, 1.0, 0.0).astype(bf)
    first_of = lax.broadcasted_iota(i32, (width, width), 0)
    second_of = lax.broadcasted_iota(i32, (width, width), 1)
    earlier = jnp.where(first_of < second_of, 1.0, 0.0).astype(bf)
    within_s[...] = mm(hot_s[...], earlier)
    sums = mm(hot_s[...], jnp.ones((width, 128), bf))
    offset = jnp.zeros((n, 128), f32)
    inverse = jnp.zeros((2 * n, 128), f32)
    lane_f = lax.broadcasted_iota(i32, (n, width), 1).astype(f32)
    slot_iota = lax.broadcasted_iota(i32, (128, width), 0)
    for b in range(blocks):
        spot = slice(b * width, (b + 1) * width)
        mine = hot_s[b * n:(b + 1) * n, :].astype(f32)
        wide_offset = jnp.concatenate([offset] * (width // 128), axis=1)
        place_in = (within_s[b * n:(b + 1) * n, :] + wide_offset) * mine
        rank = jnp.sum(place_in, axis=0, keepdims=True).astype(i32)
        rank_s[0:1, spot] = rank
        slot_hot = jnp.where(slot_iota == rank, 1.0, 0.0).astype(bf)
        named = jnp.concatenate([mine * lane_f, mine * float(b)], axis=0).astype(bf)
        inverse = inverse + mm_t(named, slot_hot)
        offset = offset + sums[b * n:(b + 1) * n, :]
    source = (inverse[0:n] + float(width) * inverse[n:2 * n]).astype(i32)
    tile_of, lane_of = source // 128, lax.rem(source, 128)
    found = [jnp.zeros((n, 128), f32) for _ in range(4)]
    for t in range(rows // 128):
        spot = slice(t * 128, (t + 1) * 128)
        here = tile_of == t
        for c in range(4):
            row = coord_ref[c:c + 1, spot] if c < 3 else elem_ref[0:1, spot].astype(f32)
            picked = jnp.take_along_axis(jnp.broadcast_to(row, (n, 128)), lane_of, axis=1)
            found[c] = jnp.where(here, picked, found[c])
    found[3] = found[3] + jnp.where(source < half_rows, float(ez), 0.0)
    for c in range(4):
        for d in range(n):
            asked[d, c:c + 1, :] = found[c][d:d + 1, 0:cap]

    pl.semaphore_wait(barrier, n - 1)

    def ask(step, carry):
        d = lax.rem(me + n // 2 + step, n)

        @pl.when(d != me)
        def _():
            pltpu.make_async_remote_copy(
                src_ref=asked.at[d], dst_ref=got.at[me], send_sem=ask_send, recv_sem=ask_recv,
                device_id=place(d), device_id_type=MESH,
            ).start()

        return carry

    lax.fori_loop(0, n, ask, 0)

    k_iota = lax.broadcasted_iota(i32, (8, ez), 0)
    e_iota = lax.broadcasted_iota(i32, (8, ez), 1)
    w_k = jnp.zeros((8, ez), f32)
    for k in range(8):
        w_k = jnp.where(k_iota == k, volume_factor * weights[k], w_k)
    joined = ((k_iota == 0) & (e_iota > 0)) | ((k_iota == 7) & (e_iota < ez - 1))
    inv_k = time_step / jnp.where(joined, 2.0 * w_k, w_k)
    inv_x = [1.0 / v for v in weights]
    inv_y = [1.0 / v for v in weights]
    inv_x[0] = jnp.where(gx > 0, 0.5, 1.0) * inv_x[0]
    inv_x[7] = jnp.where(gx < nx - 1, 0.5, 1.0) * inv_x[7]
    inv_y[0] = jnp.where(gy > 0, 0.5, 1.0) * inv_y[0]
    inv_y[7] = jnp.where(gy < ny - 1, 0.5, 1.0) * inv_y[7]
    for i in range(8):
        for j in range(8):
            wm[i, 8 * j:8 * j + 8, :] = (weights[i] * weights[j]) * w_k
            dim[i, 8 * j:8 * j + 8, :] = (inv_x[i] * inv_y[j]) * inv_k

    part = 256
    for m in range(2):
        for b in range(half_rows // part):
            spot = slice(m * half_rows + b * part, m * half_rows + (b + 1) * part)
            to = slice(b * part, (b + 1) * part)
            point = point_ref[0:1, spot]
            tall = lax.broadcasted_iota(i32, (512, part), 0)
            short = lax.broadcasted_iota(i32, (ez, part), 0)
            spread_q[m, :, to] = jnp.where(tall == point // ez, 1.0, 0.0).astype(bf)
            spread_e[m, :, to] = jnp.where(short == lax.rem(point, ez), 1.0, 0.0).astype(bf)
        held[m] = mm_t(spread_q[m], spread_e[m]).reshape(8, 64, ez)
        for i in range(8):
            held[m, i] = held[m, i] * (penalty_rate * wm[i])

    for load in loads:
        load.wait()

    def halo_copy(s, m, number):
        dx, dy = HEADINGS[number]
        lines = pl.ds(0 if dy < 0 else 56, 8)
        plane = 0 if dx < 0 else 7
        if dy == 0:
            source, target = local.at[m, plane], hx.at[s, number, m]
        elif dx == 0:
            source, target = local.at[m, :, lines, :], hy.at[s, number - 2, m]
        else:
            source, target = local.at[m, plane, lines, :], he.at[s, number - 4, m]
        return pltpu.make_async_remote_copy(
            src_ref=source, dst_ref=target, send_sem=halo_send.at[s, m, number], recv_sem=halo_recv.at[s, m, number],
            device_id=(gx + dx, gy + dy), device_id_type=MESH,
        )

    def inside(dx, dy):
        return (gx + dx >= 0) & (gx + dx < nx) & (gy + dy >= 0) & (gy + dy < ny)

    def operators(value):
        for m in range(2):
            lo = slice(m * ez, (m + 1) * ez)
            scale = nu_ref[m:m + 1, :]
            for half in range(2):
                some = slice(4 * half, 4 * half + 4)
                part = value[m, some].reshape(256, ez)
                grad[0, some, :, lo] = mm3(ops[0], ops[1], part).reshape(4, 64, ez)
                grad[1, some, :, lo] = mm3(ops[2], ops[3], part).reshape(4, 64, ez)
            for a in range(8):
                gxa = (2.0 * derivative[a][0]) * value[m, 0]
                for i in range(1, 8):
                    gxa = gxa + (2.0 * derivative[a][i]) * value[m, i]
                wma = wm[a]
                gya = grad[0, a, :, lo]
                gza = grad[1, a, :, lo]
                adv = vel[0, m, a] * gxa + vel[1, m, a] * gya + vel[2, m, a] * gza
                local[m, a] = -(wma * adv) - held[m, a] * value[m, a]
                wn = wma * scale
                work[m, a] = wn * gxa
                grad[0, a, :, lo] = wn * gya
                grad[1, a, :, lo] = wn * gza
            for half in range(2):
                some = slice(4 * half, 4 * half + 4)
                part_y = grad[0, some, :, lo].reshape(256, ez)
                part_z = grad[1, some, :, lo].reshape(256, ez)
                back = mm3(ops[4], ops[5], part_y) + mm3(ops[6], ops[7], part_z)
                local[m, some] -= back.reshape(4, 64, ez)
            for i in range(8):
                total = (2.0 * derivative[0][i]) * work[m, 0]
                for a in range(1, 8):
                    total = total + (2.0 * derivative[a][i]) * work[m, a]
                local[m, i] -= total

    operators(start)
    pltpu.make_async_copy(asked.at[me], got.at[me], in_sem.at[0]).start()
    pltpu.make_async_copy(asked.at[me], got.at[me], in_sem.at[0]).wait()
    others = got.at[pl.ds(0, n - 1)]
    pltpu.make_async_copy(others, others, ask_recv).wait()

    def prepare(g):
        wanted = jnp.concatenate([got[g * per + t] for t in range(per)], axis=1)
        wide = lax.broadcasted_iota(i32, (2 * ez, lanes), 0)
        pick[g] = jnp.where(wide == wanted[3:4].astype(i32), 1.0, 0.0).astype(bf)
        away = [wanted - v for v in gll_nodes]
        before = [None, away[0]]
        for k in range(1, 7):
            before.append(before[-1] * away[k])
        after = [None] * 7 + [None]
        after[6] = away[7]
        for k in range(5, -1, -1):
            after[k] = after[k + 1] * away[k + 1]
        for j in range(8):
            norm = 1.0
            for k in range(8):
                if k != j:
                    norm *= gll_nodes[j] - gll_nodes[k]
            factor = after[0] if j == 0 else before[7] if j == 7 else before[j] * after[j]
            factor = factor * (1.0 / norm)
            for c in range(3):
                basis_ref[g, 8 * c + j:8 * c + j + 1, :] = factor[c:c + 1]

    for s in range(3):
        value = start if s == 0 else cur
        both = jnp.concatenate([value[0].reshape(512, ez), value[1].reshape(512, ez)], axis=1)
        high, low = halves(both)

        def interpolate(p, carry):
            off = groups // 2 + ((p + 1) // 2) * (1 - 2 * lax.rem(p, 2))
            g = lax.rem(me // per + off + groups, groups)
            if s == 0:
                prepare(g)
            found = mm(high, pick[g]) + mm(low, pick[g])
            acc = found[0:64] * basis_ref[g, 0:1, :]
            for i in range(1, 8):
                acc = acc + found[64 * i:64 * i + 64] * basis_ref[g, i:i + 1, :]
            acc2 = acc[0:8] * basis_ref[g, 8:9, :]
            for j in range(1, 8):
                acc2 = acc2 + acc[8 * j:8 * j + 8] * basis_ref[g, 8 + j:9 + j, :]
            row = jnp.sum(acc2 * basis_ref[g, 16:24, :], axis=0, keepdims=True)
            for t in range(per):
                ans[s, g * per + t] = row[:, t * cap:(t + 1) * cap]
            for t in range(per):
                d = g * per + t

                @pl.when(d != me)
                def _(d=d):
                    pltpu.make_async_remote_copy(
                        src_ref=ans.at[s, d], dst_ref=rep.at[s, me],
                        send_sem=ans_send.at[s], recv_sem=ans_recv.at[s],
                        device_id=place(d), device_id_type=MESH,
                    ).start()

            return carry

        lax.fori_loop(0, groups, interpolate, 0)
        if s > 0:
            operators(cur)
        rep[s, me] = ans[s, me]
        arrived = ans.at[s, pl.ds(0, n - 1)]
        pltpu.make_async_copy(arrived, arrived, ans_recv.at[s]).wait()

        answers = jnp.concatenate([rep[s, d] for d in range(n)], axis=0)
        if cap < 128:
            answers = jnp.concatenate([answers, jnp.zeros((n, 128 - cap), f32)], axis=1)
        for m in range(2):
            pieces = []
            for t in range(half_rows // 128):
                spot = slice(m * half_rows + t * 128, m * half_rows + (t + 1) * 128)
                slot = jnp.broadcast_to(rank_s[0:1, spot], (n, 128))
                taken = jnp.take_along_axis(answers, slot, axis=1)
                own = owner_ref[0:1, spot] == lax.broadcasted_iota(i32, (n, 128), 0)
                pieces.append(jnp.sum(jnp.where(own, taken, 0.0), axis=0, keepdims=True))
            row_high, row_low = halves(jnp.concatenate(pieces, axis=1))
            where_e = spread_e[m]
            spread_v = jnp.concatenate([where_e * row_high, where_e * row_low], axis=0)
            added = mm_t(spread_q[m], spread_v)
            for i in range(8):
                rows_i = slice(64 * i, 64 * i + 64)
                local[m, i] += (penalty_rate * wm[i]) * (added[rows_i, :ez] + added[rows_i, ez:])
            lane = lax.broadcasted_iota(i32, (8, ez), 1)
            for i in range(8):
                lower = local[m, i, pl.ds(0, 8, stride=8), :]
                upper = local[m, i, pl.ds(7, 8, stride=8), :]
                shared = upper + pltpu.roll(lower, ez - 1, 1)
                local[m, i, pl.ds(7, 8, stride=8), :] = jnp.where(lane < ez - 1, shared, upper)
                local[m, i, pl.ds(0, 8, stride=8), :] = jnp.where(lane > 0, pltpu.roll(shared, 1, 1), lower)
            for number, (dx, dy) in enumerate(HEADINGS):
                @pl.when(inside(dx, dy))
                def _(m=m, number=number):
                    halo_copy(s, m, number).start()

        target = cur if s < 2 else out_ref
        share = (1.0, 0.25, 2.0 / 3.0)[s]
        for m in range(2):
            for i in range(8):
                moved = value[m, i] + local[m, i] * dim[i]
                if s == 0:
                    cur[m, i] = moved
                elif s == 1:
                    cur[m, i] = 0.75 * start[m, i] + 0.25 * moved
                else:
                    out_ref[m, i] = start[m, i] * (1.0 / 3.0) + (2.0 / 3.0) * moved
        for m in range(2):
            for number, (dx, dy) in enumerate(HEADINGS):
                @pl.when(inside(-dx, -dy))
                def _(m=m, number=number, dx=dx, dy=dy):
                    halo_copy(s, m, number).wait_recv()
                    plane = 7 if dx < 0 else 0
                    lines = slice(56, 64) if dy < 0 else slice(0, 8)
                    if dy == 0:
                        target[m, plane] += hx[s, number, m] * (share * dim[plane])
                    elif dx == 0:
                        target[m, :, lines, :] += hy[s, number - 2, m] * (share * dim[:, lines, :])
                    else:
                        target[m, plane, lines, :] += he[s, number - 4, m] * (share * dim[plane, lines, :])
        for m in range(2):
            for number, (dx, dy) in enumerate(HEADINGS):
                @pl.when(inside(dx, dy))
                def _(m=m, number=number):
                    halo_copy(s, m, number).wait_send()

    sent = got.at[pl.ds(0, n - 1)]
    pltpu.make_async_copy(sent, sent, ask_send).wait()
    for s in range(3):
        whole = ans.at[s, pl.ds(0, n - 1)]
        pltpu.make_async_copy(whole, whole, ans_send.at[s]).wait()


def split_host(matrix):
    high = matrix.astype(jnp.bfloat16)
    low = (matrix - high.astype(np.float64)).astype(jnp.bfloat16)
    return [high, low]


def body(scalar, velocity, diffusivity, recv_owner, donor_elem, recv_point, recv_coords):
    tables = gll_tables()
    derivative = tables[2]
    ez = scalar.shape[4]
    n = lax.axis_size("gx") * lax.axis_size("gy")
    rows = recv_owner.shape[0]
    cap = max(2, 2 * rows // n)
    per = max(1, min(n, 512 // cap))
    groups, lanes = n // per, per * cap
    width = min(256, rows)
    blocks = rows // width
    bf, f32, i32 = jnp.bfloat16, jnp.float32, jnp.int32

    half_eye = np.eye(4)
    table = 2.0 * np.asarray(derivative, np.float64)
    along_y = np.kron(half_eye, np.kron(table, np.eye(8)))
    along_z = np.kron(half_eye, np.kron(np.eye(8), table))
    ops = []
    for matrix in (along_y, along_z, along_y.T, along_z.T):
        ops = ops + split_host(matrix)
    ops = jnp.asarray(np.stack(ops))

    vmem = pltpu.VMEM
    dma = pltpu.SemaphoreType.DMA
    field = (2, 8, 64, ez)
    in_vmem, anywhere = pl.BlockSpec(memory_space=vmem), pl.BlockSpec(memory_space=pl.ANY)
    out = pl.pallas_call(
        functools.partial(step_kernel, tables),
        out_shape=jax.ShapeDtypeStruct(field, f32),
        in_specs=[in_vmem] * 5 + [anywhere] * 3,
        out_specs=in_vmem,
        scratch_shapes=[
            vmem(field, f32),
            vmem((3,) + field, f32),
            vmem((8, 256, 256), bf),
            vmem(field, f32),
            vmem(field, f32),
            vmem(field, f32),
            vmem((2, 8, 64, 2 * ez), f32),
            vmem((8, 64, ez), f32),
            vmem((8, 64, ez), f32),
            vmem(field, f32),
            vmem((blocks * n, width), bf),
            vmem((blocks * n, width), f32),
            vmem((1, rows), i32),
            vmem((n, 4, cap), f32),
            vmem((n, 4, cap), f32),
            vmem((groups, 2 * ez, lanes), bf),
            vmem((groups, 24, lanes), f32),
            vmem((2, 512, rows // 2), bf),
            vmem((2, ez, rows // 2), bf),
            vmem((3, n, 1, cap), f32),
            vmem((3, n, 1, cap), f32),
            vmem((3, 2, 2, 64, ez), f32),
            vmem((3, 2, 2, 8, 8, ez), f32),
            vmem((3, 4, 2, 8, ez), f32),
            dma((3,)),
            dma,
            dma,
            dma((3,)),
            dma((3,)),
            dma((3, 2, 8)),
            dma((3, 2, 8)),
        ],
        compiler_params=pltpu.CompilerParams(collective_id=0, has_side_effects=True),
        name="advance",
    )(
        recv_owner.reshape(1, rows), donor_elem.reshape(1, rows), recv_point.reshape(1, rows), recv_coords,
        diffusivity.reshape(2, ez), scalar.reshape(field), velocity.reshape((3,) + field), ops,
    )
    return out.reshape(scalar.shape)


def solution(mesh):
    return jax.shard_map(
        body,
        mesh=mesh,
        in_specs=(
            P(None, None, "gx", "gy", None),
            P(None, None, None, "gx", "gy", None),
            P(None, "gx", "gy", None),
            P(("gx", "gy"), None),
            P(("gx", "gy")),
            P(("gx", "gy")),
            P(None, ("gx", "gy")),
        ),
        out_specs=P(None, None, "gx", "gy", None),
        check_vma=False,
    )
```

```python
import functools
import jax
import jax.numpy as jnp
import numpy as np
from jax import lax
from jax.experimental import pallas as pl
from jax.experimental.pallas import tpu as pltpu
from jax.sharding import PartitionSpec as P

time_step = 0.01
penalty_rate = 50.0
volume_factor = 0.125
node_inner = [0.8717401485096066, 0.5917001814331423, 0.20929921790247888]


def legendre_seven(point):
    before, current = (1.0, point)
    for order in range(1, 7):
        before, current = (
            current,
            ((2 * order + 1) * point * current - order * before) / (order + 1),
        )
    return current


def gll_tables():
    degree = 7
    gll_nodes = [-1.0] + [-v for v in node_inner] + node_inner[::-1] + [1.0]
    end_values = [legendre_seven(v) for v in gll_nodes]
    weights = [2.0 / (degree * (degree + 1) * v * v) for v in end_values]
    derivative = [[0.0] * 8 for _ in range(8)]
    for a in range(8):
        for b in range(8):
            if a != b:
                derivative[a][b] = end_values[a] / (end_values[b] * (gll_nodes[a] - gll_nodes[b]))
    derivative[0][0] = -degree * (degree + 1) / 4.0
    derivative[7][7] = degree * (degree + 1) / 4.0
    return (gll_nodes, weights, derivative)


MESH = pl.DeviceIdType.MESH
HEADINGS = [(-1, 0), (1, 0), (0, -1), (0, 1), (-1, -1), (-1, 1), (1, -1), (1, 1)]
INNER = range(1, 7)
FACE = [(i, j) for i in (0, 7) for j in range(8)] + [(i, j) for j in (0, 7) for i in INNER]
INTERIOR = [(i, j) for i in INNER for j in INNER]


def halves(value):
    high = value.astype(jnp.bfloat16)
    return high, (value - high.astype(jnp.float32)).astype(jnp.bfloat16)


def mm(a, b):
    return jnp.dot(a, b, preferred_element_type=jnp.float32)


def mm_t(a, b):
    return lax.dot_general(a, b, (((1,), (1,)), ((), ())), preferred_element_type=jnp.float32)


def mm3(op_high, op_low, value):
    high, low = halves(value)
    return mm(op_high, high) + mm(op_high, low) + mm(op_low, high)


def step_kernel(
    tables, owner_ref, elem_ref, point_ref, coord_ref, nu_ref, start_hbm, vel_hbm, ops_hbm,
    out_ref,
    start, vel, ops, cur, local, work, grad, wm, dim, held,
    hot_s, within_s, rank_s, asked, got, pick, basis_ref, spread_q, spread_e,
    ans, rep, hx, hy, he, lhs_face, lhs_inner, inner_part,
    in_sem, ask_send, ask_recv, ans_send, ans_recv, halo_send, halo_recv,
):
    gll_nodes, weights, derivative = tables
    f32, bf, i32 = jnp.float32, jnp.bfloat16, jnp.int32
    gx, gy = lax.axis_index("gx"), lax.axis_index("gy")
    nx, ny = lax.axis_size("gx"), lax.axis_size("gy")
    n = nx * ny
    me = gx * ny + gy
    ez = start.shape[-1]
    rows = owner_ref.shape[-1]
    cap = ans.shape[-1]
    groups, _, lanes = pick.shape
    per = lanes // cap
    width = within_s.shape[-1]
    blocks = rows // width
    half_rows = rows // 2

    barrier = pltpu.get_barrier_semaphore()

    def place(d):
        return (d // ny, lax.rem(d, ny))

    def greet(a, carry):
        px = lax.rem(gx + nx // 2 + a, nx)
        for b in range(ny):
            @pl.when((px != gx) | (gy != b))
            def _(b=b):
                pl.semaphore_signal(barrier, inc=1, device_id=(px, b), device_id_type=MESH)

        return carry

    lax.fori_loop(0, nx, greet, 0)
    loads = [
        pltpu.make_async_copy(start_hbm, start, in_sem.at[0]),
        pltpu.make_async_copy(vel_hbm, vel, in_sem.at[1]),
        pltpu.make_async_copy(ops_hbm, ops, in_sem.at[2]),
    ]
    for load in loads:
        load.start()

    for b in range(blocks):
        spot = slice(b * width, (b + 1) * width)
        iota_n = lax.broadcasted_iota(i32, (n, width), 0)
        hot_s[b * n:(b + 1) * n, :] = jnp.where(owner_ref[0:1, spot] == iota_n, 1.0, 0.0).astype(bf)
    first_of = lax.broadcasted_iota(i32, (width, width), 0)
    second_of = lax.broadcasted_iota(i32, (width, width), 1)
    earlier = jnp.where(first_of < second_of, 1.0, 0.0).astype(bf)
    within_s[...] = mm(hot_s[...], earlier)
    sums = mm(hot_s[...], jnp.ones((width, 128), bf))
    offset = jnp.zeros((n, 128), f32)
    inverse = jnp.zeros((2 * n, 128), f32)
    lane_f = lax.broadcasted_iota(i32, (n, width), 1).astype(f32)
    slot_iota = lax.broadcasted_iota(i32, (128, width), 0)
    for b in range(blocks):
        spot = slice(b * width, (b + 1) * width)
        mine = hot_s[b * n:(b + 1) * n, :].astype(f32)
        wide_offset = jnp.concatenate([offset] * (width // 128), axis=1)
        place_in = (within_s[b * n:(b + 1) * n, :] + wide_offset) * mine
        rank = jnp.sum(place_in, axis=0, keepdims=True).astype(i32)
        rank_s[0:1, spot] = rank
        slot_hot = jnp.where(slot_iota == rank, 1.0, 0.0).astype(bf)
        named = jnp.concatenate([mine * lane_f, mine * float(b)], axis=0).astype(bf)
        inverse = inverse + mm_t(named, slot_hot)
        offset = offset + sums[b * n:(b + 1) * n, :]
    source = (inverse[0:n] + float(width) * inverse[n:2 * n]).astype(i32)
    tile_of, lane_of = source // 128, lax.rem(source, 128)
    found = [jnp.zeros((n, 128), f32) for _ in range(4)]
    for t in range(rows // 128):
        spot = slice(t * 128, (t + 1) * 128)
        here = tile_of == t
        for c in range(4):
            row = coord_ref[c:c + 1, spot] if c < 3 else elem_ref[0:1, spot].astype(f32)
            picked = jnp.take_along_axis(jnp.broadcast_to(row, (n, 128)), lane_of, axis=1)
            found[c] = jnp.where(here, picked, found[c])
    found[3] = found[3] + jnp.where(source < half_rows, float(ez), 0.0)
    for c in range(4):
        for d in range(n):
            asked[d, c:c + 1, :] = found[c][d:d + 1, 0:cap]

    pl.semaphore_wait(barrier, n - 1)

    own_group = me // per

    def ask(a, carry):
        px = lax.rem(gx + nx // 2 + a, nx)
        for b in range(ny):
            @pl.when((px != gx) | (gy != b))
            def _(b=b):
                pltpu.make_async_remote_copy(
                    src_ref=asked.at[px * ny + b], dst_ref=got.at[me],
                    send_sem=ask_send, recv_sem=ask_recv.at[own_group],
                    device_id=(px, b), device_id_type=MESH,
                ).start()

        return carry

    lax.fori_loop(0, nx, ask, 0)

    k_iota = lax.broadcasted_iota(i32, (8, ez), 0)
    e_iota = lax.broadcasted_iota(i32, (8, ez), 1)
    w_k = jnp.zeros((8, ez), f32)
    for k in range(8):
        w_k = jnp.where(k_iota == k, volume_factor * weights[k], w_k)
    joined = ((k_iota == 0) & (e_iota > 0)) | ((k_iota == 7) & (e_iota < ez - 1))
    inv_k = time_step / jnp.where(joined, 2.0 * w_k, w_k)
    inv_x = [1.0 / v for v in weights]
    inv_y = [1.0 / v for v in weights]
    inv_x[0] = jnp.where(gx > 0, 0.5, 1.0) * inv_x[0]
    inv_x[7] = jnp.where(gx < nx - 1, 0.5, 1.0) * inv_x[7]
    inv_y[0] = jnp.where(gy > 0, 0.5, 1.0) * inv_y[0]
    inv_y[7] = jnp.where(gy < ny - 1, 0.5, 1.0) * inv_y[7]
    for i in range(8):
        for j in range(8):
            wm[i, 8 * j:8 * j + 8, :] = (weights[i] * weights[j]) * w_k
            dim[i, 8 * j:8 * j + 8, :] = (inv_x[i] * inv_y[j]) * inv_k

    part = 256
    for m in range(2):
        for b in range(half_rows // part):
            spot = slice(m * half_rows + b * part, m * half_rows + (b + 1) * part)
            to = slice(b * part, (b + 1) * part)
            point = point_ref[0:1, spot]
            eight = lax.broadcasted_iota(i32, (8, part), 0)
            tall = jnp.concatenate([eight + (64 * i + 8 * j) for i, j in FACE + INTERIOR], axis=0)
            short = lax.broadcasted_iota(i32, (ez, part), 0)
            spread_q[m, :, to] = jnp.where(tall == point // ez, 1.0, 0.0).astype(bf)
            spread_e[m, :, to] = jnp.where(short == lax.rem(point, ez), 1.0, 0.0).astype(bf)
        count = mm_t(spread_q[m], spread_e[m])
        for at, (i, j) in enumerate(FACE + INTERIOR):
            spot = slice(8 * j, 8 * j + 8)
            held[m, i, spot] = count[8 * at:8 * at + 8] * (penalty_rate * wm[i, spot])

    for load in loads:
        load.wait()

    def halo_copy(s, m, number):
        dx, dy = HEADINGS[number]
        lines = pl.ds(0 if dy < 0 else 56, 8)
        plane = 0 if dx < 0 else 7
        if dy == 0:
            source, target = local.at[m, plane], hx.at[s, number, m]
        elif dx == 0:
            source, target = local.at[m, :, lines, :], hy.at[s, number - 2, m]
        else:
            source, target = local.at[m, plane, lines, :], he.at[s, number - 4, m]
        return pltpu.make_async_remote_copy(
            src_ref=source, dst_ref=target, send_sem=halo_send.at[s, m, number], recv_sem=halo_recv.at[s, m, number],
            device_id=(gx + dx, gy + dy), device_id_type=MESH,
        )

    def inside(dx, dy):
        return (gx + dx >= 0) & (gx + dx < nx) & (gy + dy >= 0) & (gy + dy < ny)

    def operators(value):
        for m in range(2):
            lo = slice(m * ez, (m + 1) * ez)
            scale = nu_ref[m:m + 1, :]
            for half in range(2):
                some = slice(4 * half, 4 * half + 4)
                part = value[m, some].reshape(256, ez)
                grad[0, some, :, lo] = mm3(ops[0], ops[1], part).reshape(4, 64, ez)
                grad[1, some, :, lo] = mm3(ops[2], ops[3], part).reshape(4, 64, ez)
            for a in range(8):
                gxa = (2.0 * derivative[a][0]) * value[m, 0]
                for i in range(1, 8):
                    gxa = gxa + (2.0 * derivative[a][i]) * value[m, i]
                wma = wm[a]
                gya = grad[0, a, :, lo]
                gza = grad[1, a, :, lo]
                adv = vel[0, m, a] * gxa + vel[1, m, a] * gya + vel[2, m, a] * gza
                local[m, a] = -(wma * adv) - held[m, a] * value[m, a]
                wn = wma * scale
                work[m, a] = wn * gxa
                grad[0, a, :, lo] = wn * gya
                grad[1, a, :, lo] = wn * gza
            for half in range(2):
                some = slice(4 * half, 4 * half + 4)
                part_y = grad[0, some, :, lo].reshape(256, ez)
                part_z = grad[1, some, :, lo].reshape(256, ez)
                back = mm3(ops[4], ops[5], part_y) + mm3(ops[6], ops[7], part_z)
                local[m, some] -= back.reshape(4, 64, ez)
            for i in range(8):
                total = (2.0 * derivative[0][i]) * work[m, 0]
                for a in range(1, 8):
                    total = total + (2.0 * derivative[a][i]) * work[m, a]
                local[m, i] -= total

    operators(start)
    pltpu.make_async_copy(asked.at[me], got.at[me], in_sem.at[0]).start()
    pltpu.make_async_copy(asked.at[me], got.at[me], in_sem.at[0]).wait()
    def prepare(g):
        wanted = jnp.concatenate([got[g * per + t] for t in range(per)], axis=1)
        wide = lax.broadcasted_iota(i32, (2 * ez, lanes), 0)
        pick[g] = jnp.where(wide == wanted[3:4].astype(i32), 1.0, 0.0).astype(bf)
        away = [wanted - v for v in gll_nodes]
        before = [None, away[0]]
        for k in range(1, 7):
            before.append(before[-1] * away[k])
        after = [None] * 7 + [None]
        after[6] = away[7]
        for k in range(5, -1, -1):
            after[k] = after[k + 1] * away[k + 1]
        for j in range(8):
            norm = 1.0
            for k in range(8):
                if k != j:
                    norm *= gll_nodes[j] - gll_nodes[k]
            factor = after[0] if j == 0 else before[7] if j == 7 else before[j] * after[j]
            factor = factor * (1.0 / norm)
            for c in range(3):
                basis_ref[g, 8 * c + j:8 * c + j + 1, :] = factor[c:c + 1]

    nearby = got.at[pl.ds(0, per - 1)]
    pltpu.make_async_copy(nearby, nearby, ask_recv.at[own_group]).wait()
    prepare(own_group)

    def next_group(p, carry):
        off = ((p + 1) // 2) * (1 - 2 * lax.rem(p, 2))
        g = lax.rem(own_group + off + groups, groups)
        some = got.at[pl.ds(0, per)]
        pltpu.make_async_copy(some, some, ask_recv.at[g]).wait()
        prepare(g)
        return carry

    lax.fori_loop(1, groups, next_group, 0)

    def split_lines(value, lines, into):
        both = jnp.concatenate(
            [jnp.concatenate([value[m, i, 8 * j:8 * j + 8] for i, j in lines], axis=0) for m in range(2)], axis=1
        )
        into[0], into[1] = halves(both)

    def contract(lines, lhs, g):
        found = mm(lhs[0], pick[g]) + mm(lhs[1], pick[g])
        total = None
        for j in range(8):
            line = None
            for at, (i, jj) in enumerate(lines):
                if jj == j:
                    term = found[8 * at:8 * at + 8] * basis_ref[g, i:i + 1, :]
                    line = term if line is None else line + term
            if line is not None:
                line = line * basis_ref[g, 8 + j:9 + j, :]
                total = line if total is None else total + line
        return total

    def sum_third(flat, m, first, size, stride):
        lane = lax.broadcasted_iota(i32, (size, ez), 1)
        low_rows, high_rows = pl.ds(first, size, stride=stride), pl.ds(first + 7, size, stride=stride)
        lower, upper = flat[m, low_rows, :], flat[m, high_rows, :]
        shared = upper + pltpu.roll(lower, ez - 1, 1)
        flat[m, high_rows, :] = jnp.where(lane < ez - 1, shared, upper)
        flat[m, low_rows, :] = jnp.where(lane > 0, pltpu.roll(shared, 1, 1), lower)

    flat = local.reshape(2, 512, ez)

    for s in range(3):
        value = start if s == 0 else cur
        if s == 0:
            split_lines(start, INTERIOR, lhs_inner)
        split_lines(value, FACE, lhs_face)

        def interpolate(p, carry):
            off = groups // 2 + ((p + 1) // 2) * (1 - 2 * lax.rem(p, 2))
            g = lax.rem(own_group + off + groups, groups)
            total = contract(FACE, lhs_face, g)
            total = total + (contract(INTERIOR, lhs_inner, g) if s == 0 else inner_part[g])
            row = jnp.sum(total * basis_ref[g, 16:24, :], axis=0, keepdims=True)
            for t in range(per):
                ans[s, g * per + t] = row[:, t * cap:(t + 1) * cap]
            for t in range(per):
                d = g * per + t

                @pl.when(d != me)
                def _(d=d):
                    pltpu.make_async_remote_copy(
                        src_ref=ans.at[s, d], dst_ref=rep.at[s, me],
                        send_sem=ans_send.at[s], recv_sem=ans_recv.at[s],
                        device_id=place(d), device_id_type=MESH,
                    ).start()

            return carry

        lax.fori_loop(0, groups, interpolate, 0)
        if s > 0:
            operators(cur)
        rep[s, me] = ans[s, me]
        arrived = ans.at[s, pl.ds(0, n - 1)]
        pltpu.make_async_copy(arrived, arrived, ans_recv.at[s]).wait()

        answers = jnp.concatenate([rep[s, d] for d in range(n)], axis=0)
        if cap < 128:
            answers = jnp.concatenate([answers, jnp.zeros((n, 128 - cap), f32)], axis=1)

        def scatter(m, lines, first):
            added = mm_t(spread_q[m, first:first + 8 * len(lines), :], spread_v[m])
            for at, (i, j) in enumerate(lines):
                spot, rows_at = slice(8 * j, 8 * j + 8), slice(8 * at, 8 * at + 8)
                local[m, i, spot] += (penalty_rate * wm[i, spot]) * (added[rows_at, :ez] + added[rows_at, ez:])

        spread_v = []
        for m in range(2):
            pieces = []
            for t in range(half_rows // 128):
                spot = slice(m * half_rows + t * 128, m * half_rows + (t + 1) * 128)
                slot = jnp.broadcast_to(rank_s[0:1, spot], (n, 128))
                taken = jnp.take_along_axis(answers, slot, axis=1)
                own = owner_ref[0:1, spot] == lax.broadcasted_iota(i32, (n, 128), 0)
                pieces.append(jnp.sum(jnp.where(own, taken, 0.0), axis=0, keepdims=True))
            row_high, row_low = halves(jnp.concatenate(pieces, axis=1))
            where_e = spread_e[m]
            spread_v.append(jnp.concatenate([where_e * row_high, where_e * row_low], axis=0))
            scatter(m, FACE, 0)
            for i in (0, 7):
                sum_third(flat, m, 64 * i + 8, 6, 8)
            for j in (0, 7):
                sum_third(flat, m, 8 * j, 8, 64)
            for number, (dx, dy) in enumerate(HEADINGS):
                @pl.when(inside(dx, dy))
                def _(m=m, number=number):
                    halo_copy(s, m, number).start()

        target = cur if s < 2 else out_ref
        share = (1.0, 0.25, 2.0 / 3.0)[s]
        for m in range(2):
            scatter(m, INTERIOR, 8 * len(FACE))
            for i in INNER:
                sum_third(flat, m, 64 * i + 8, 6, 8)
            for i in range(8):
                moved = value[m, i] + local[m, i] * dim[i]
                if s == 0:
                    cur[m, i] = moved
                elif s == 1:
                    cur[m, i] = 0.75 * start[m, i] + 0.25 * moved
                else:
                    out_ref[m, i] = start[m, i] * (1.0 / 3.0) + (2.0 / 3.0) * moved
        if s < 2:
            split_lines(cur, INTERIOR, lhs_inner)

            def ahead(g, carry):
                inner_part[g] = contract(INTERIOR, lhs_inner, g)
                return carry

            lax.fori_loop(0, groups, ahead, 0)
        for m in range(2):
            for number, (dx, dy) in enumerate(HEADINGS):
                @pl.when(inside(-dx, -dy))
                def _(m=m, number=number, dx=dx, dy=dy):
                    halo_copy(s, m, number).wait_recv()
                    plane = 7 if dx < 0 else 0
                    lines = slice(56, 64) if dy < 0 else slice(0, 8)
                    if dy == 0:
                        target[m, plane] += hx[s, number, m] * (share * dim[plane])
                    elif dx == 0:
                        target[m, :, lines, :] += hy[s, number - 2, m] * (share * dim[:, lines, :])
                    else:
                        target[m, plane, lines, :] += he[s, number - 4, m] * (share * dim[plane, lines, :])
        for m in range(2):
            for number, (dx, dy) in enumerate(HEADINGS):
                @pl.when(inside(dx, dy))
                def _(m=m, number=number):
                    halo_copy(s, m, number).wait_send()

    sent = got.at[pl.ds(0, n - 1)]
    pltpu.make_async_copy(sent, sent, ask_send).wait()
    for s in range(3):
        whole = ans.at[s, pl.ds(0, n - 1)]
        pltpu.make_async_copy(whole, whole, ans_send.at[s]).wait()


def split_host(matrix):
    high = matrix.astype(jnp.bfloat16)
    low = (matrix - high.astype(np.float64)).astype(jnp.bfloat16)
    return [high, low]


def body(scalar, velocity, diffusivity, recv_owner, donor_elem, recv_point, recv_coords):
    tables = gll_tables()
    derivative = tables[2]
    ez = scalar.shape[4]
    n = lax.axis_size("gx") * lax.axis_size("gy")
    rows = recv_owner.shape[0]
    cap = max(2, 2 * rows // n)
    per = max(1, min(n, 512 // cap))
    groups, lanes = n // per, per * cap
    width = min(256, rows)
    blocks = rows // width
    bf, f32, i32 = jnp.bfloat16, jnp.float32, jnp.int32

    half_eye = np.eye(4)
    table = 2.0 * np.asarray(derivative, np.float64)
    along_y = np.kron(half_eye, np.kron(table, np.eye(8)))
    along_z = np.kron(half_eye, np.kron(np.eye(8), table))
    ops = []
    for matrix in (along_y, along_z, along_y.T, along_z.T):
        ops = ops + split_host(matrix)
    ops = jnp.asarray(np.stack(ops))

    vmem = pltpu.VMEM
    dma = pltpu.SemaphoreType.DMA
    field = (2, 8, 64, ez)
    in_vmem, anywhere = pl.BlockSpec(memory_space=vmem), pl.BlockSpec(memory_space=pl.ANY)
    out = pl.pallas_call(
        functools.partial(step_kernel, tables),
        out_shape=jax.ShapeDtypeStruct(field, f32),
        in_specs=[in_vmem] * 5 + [anywhere] * 3,
        out_specs=in_vmem,
        scratch_shapes=[
            vmem(field, f32),
            vmem((3,) + field, f32),
            vmem((8, 256, 256), bf),
            vmem(field, f32),
            vmem(field, f32),
            vmem(field, f32),
            vmem((2, 8, 64, 2 * ez), f32),
            vmem((8, 64, ez), f32),
            vmem((8, 64, ez), f32),
            vmem(field, f32),
            vmem((blocks * n, width), bf),
            vmem((blocks * n, width), f32),
            vmem((1, rows), i32),
            vmem((n, 4, cap), f32),
            vmem((n, 4, cap), f32),
            vmem((groups, 2 * ez, lanes), bf),
            vmem((groups, 24, lanes), f32),
            vmem((2, 512, rows // 2), bf),
            vmem((2, ez, rows // 2), bf),
            vmem((3, n, 1, cap), f32),
            vmem((3, n, 1, cap), f32),
            vmem((3, 2, 2, 64, ez), f32),
            vmem((3, 2, 2, 8, 8, ez), f32),
            vmem((3, 4, 2, 8, ez), f32),
            vmem((2, 8 * len(FACE), 2 * ez), bf),
            vmem((2, 8 * len(INTERIOR), 2 * ez), bf),
            vmem((groups, 8, lanes), f32),
            dma((3,)),
            dma,
            dma((groups,)),
            dma((3,)),
            dma((3,)),
            dma((3, 2, 8)),
            dma((3, 2, 8)),
        ],
        compiler_params=pltpu.CompilerParams(collective_id=0, has_side_effects=True),
        name="advance",
    )(
        recv_owner.reshape(1, rows), donor_elem.reshape(1, rows), recv_point.reshape(1, rows), recv_coords,
        diffusivity.reshape(2, ez), scalar.reshape(field), velocity.reshape((3,) + field), ops,
    )
    return out.reshape(scalar.shape)


def solution(mesh):
    return jax.shard_map(
        body,
        mesh=mesh,
        in_specs=(
            P(None, None, "gx", "gy", None),
            P(None, None, None, "gx", "gy", None),
            P(None, "gx", "gy", None),
            P(("gx", "gy"), None),
            P(("gx", "gy")),
            P(("gx", "gy")),
            P(None, ("gx", "gy")),
        ),
        out_specs=P(None, None, "gx", "gy", None),
        check_vma=False,
    )
```

```python
import functools
import jax
import jax.numpy as jnp
import numpy as np
from jax import lax
from jax.experimental import pallas as pl
from jax.experimental.pallas import tpu as pltpu
from jax.sharding import PartitionSpec as P

time_step = 0.01
penalty_rate = 50.0
volume_factor = 0.125
node_inner = [0.8717401485096066, 0.5917001814331423, 0.20929921790247888]


def legendre_seven(point):
    before, current = (1.0, point)
    for order in range(1, 7):
        before, current = (
            current,
            ((2 * order + 1) * point * current - order * before) / (order + 1),
        )
    return current


def gll_tables():
    degree = 7
    gll_nodes = [-1.0] + [-v for v in node_inner] + node_inner[::-1] + [1.0]
    end_values = [legendre_seven(v) for v in gll_nodes]
    weights = [2.0 / (degree * (degree + 1) * v * v) for v in end_values]
    derivative = [[0.0] * 8 for _ in range(8)]
    for a in range(8):
        for b in range(8):
            if a != b:
                derivative[a][b] = end_values[a] / (end_values[b] * (gll_nodes[a] - gll_nodes[b]))
    derivative[0][0] = -degree * (degree + 1) / 4.0
    derivative[7][7] = degree * (degree + 1) / 4.0
    return (gll_nodes, weights, derivative)


MESH = pl.DeviceIdType.MESH
HEADINGS = [(-1, 0), (1, 0), (0, -1), (0, 1), (-1, -1), (-1, 1), (1, -1), (1, 1)]
INNER = range(1, 7)
FACE = [(i, j) for i in (0, 7) for j in range(8)] + [(i, j) for j in (0, 7) for i in INNER]
INTERIOR = [(i, j) for i in INNER for j in INNER]


def halves(value):
    high = value.astype(jnp.bfloat16)
    return high, (value - high.astype(jnp.float32)).astype(jnp.bfloat16)


def mm(a, b):
    return jnp.dot(a, b, preferred_element_type=jnp.float32)


def mm_t(a, b):
    return lax.dot_general(a, b, (((1,), (1,)), ((), ())), preferred_element_type=jnp.float32)


def mm3(op_high, op_low, value):
    high, low = halves(value)
    return mm(op_high, high) + mm(op_high, low) + mm(op_low, high)


def step_kernel(
    tables, owner_ref, elem_ref, point_ref, coord_ref, nu_ref, start_hbm, vel_hbm, ops_hbm,
    out_ref,
    start, vel, ops, cur, local, work, grad, wm, dim, held,
    hot_s, within_s, rank_s, asked, got, pick, basis_ref, spread_q, spread_e,
    ans, rep, hx, hy, he, lhs, inner_part,
    in_sem, ask_send, ask_recv, ans_send, ans_recv, halo_send, halo_recv,
):
    gll_nodes, weights, derivative = tables
    f32, bf, i32 = jnp.float32, jnp.bfloat16, jnp.int32
    gx, gy = lax.axis_index("gx"), lax.axis_index("gy")
    nx, ny = lax.axis_size("gx"), lax.axis_size("gy")
    n = nx * ny
    me = gx * ny + gy
    ez = start.shape[-1]
    rows = owner_ref.shape[-1]
    cap = ans.shape[-1]
    groups, _, lanes = pick.shape
    per = lanes // cap
    width = within_s.shape[-1]
    blocks = rows // width
    half_rows = rows // 2

    barrier = pltpu.get_barrier_semaphore()

    def place(d):
        return (d // ny, lax.rem(d, ny))

    def greet(a, carry):
        px = lax.rem(gx + nx // 2 + a, nx)
        for b in range(ny):
            @pl.when((px != gx) | (gy != b))
            def _(b=b):
                pl.semaphore_signal(barrier, inc=1, device_id=(px, b), device_id_type=MESH)

        return carry

    lax.fori_loop(0, nx, greet, 0)
    loads = [
        pltpu.make_async_copy(start_hbm, start, in_sem.at[0]),
        pltpu.make_async_copy(vel_hbm, vel, in_sem.at[1]),
        pltpu.make_async_copy(ops_hbm, ops, in_sem.at[2]),
    ]
    for load in loads:
        load.start()

    for b in range(blocks):
        spot = slice(b * width, (b + 1) * width)
        iota_n = lax.broadcasted_iota(i32, (n, width), 0)
        hot_s[b * n:(b + 1) * n, :] = jnp.where(owner_ref[0:1, spot] == iota_n, 1.0, 0.0).astype(bf)
    first_of = lax.broadcasted_iota(i32, (width, width), 0)
    second_of = lax.broadcasted_iota(i32, (width, width), 1)
    earlier = jnp.where(first_of < second_of, 1.0, 0.0).astype(bf)
    within_s[...] = mm(hot_s[...], earlier)
    sums = mm(hot_s[...], jnp.ones((width, 128), bf))
    offset = jnp.zeros((n, 128), f32)
    inverse = jnp.zeros((2 * n, 128), f32)
    lane_f = lax.broadcasted_iota(i32, (n, width), 1).astype(f32)
    slot_iota = lax.broadcasted_iota(i32, (128, width), 0)
    for b in range(blocks):
        spot = slice(b * width, (b + 1) * width)
        mine = hot_s[b * n:(b + 1) * n, :].astype(f32)
        wide_offset = jnp.concatenate([offset] * (width // 128), axis=1)
        place_in = (within_s[b * n:(b + 1) * n, :] + wide_offset) * mine
        rank = jnp.sum(place_in, axis=0, keepdims=True).astype(i32)
        rank_s[0:1, spot] = rank
        slot_hot = jnp.where(slot_iota == rank, 1.0, 0.0).astype(bf)
        named = jnp.concatenate([mine * lane_f, mine * float(b)], axis=0).astype(bf)
        inverse = inverse + mm_t(named, slot_hot)
        offset = offset + sums[b * n:(b + 1) * n, :]
    source = (inverse[0:n] + float(width) * inverse[n:2 * n]).astype(i32)
    tile_of, lane_of = source // 128, lax.rem(source, 128)
    found = [jnp.zeros((n, 128), f32) for _ in range(4)]
    for t in range(rows // 128):
        spot = slice(t * 128, (t + 1) * 128)
        here = tile_of == t
        for c in range(4):
            row = coord_ref[c:c + 1, spot] if c < 3 else elem_ref[0:1, spot].astype(f32)
            picked = jnp.take_along_axis(jnp.broadcast_to(row, (n, 128)), lane_of, axis=1)
            found[c] = jnp.where(here, picked, found[c])
    found[3] = found[3] + jnp.where(source < half_rows, float(ez), 0.0)
    for c in range(4):
        for d in range(n):
            asked[d, c:c + 1, :] = found[c][d:d + 1, 0:cap]

    pl.semaphore_wait(barrier, n - 1)

    own_group = me // per

    def ask(a, carry):
        px = lax.rem(gx + nx // 2 + a, nx)
        for b in range(ny):
            @pl.when((px != gx) | (gy != b))
            def _(b=b):
                pltpu.make_async_remote_copy(
                    src_ref=asked.at[px * ny + b], dst_ref=got.at[me],
                    send_sem=ask_send, recv_sem=ask_recv.at[own_group],
                    device_id=(px, b), device_id_type=MESH,
                ).start()

        return carry

    lax.fori_loop(0, nx, ask, 0)

    k_iota = lax.broadcasted_iota(i32, (8, ez), 0)
    e_iota = lax.broadcasted_iota(i32, (8, ez), 1)
    w_k = jnp.zeros((8, ez), f32)
    for k in range(8):
        w_k = jnp.where(k_iota == k, volume_factor * weights[k], w_k)
    joined = ((k_iota == 0) & (e_iota > 0)) | ((k_iota == 7) & (e_iota < ez - 1))
    inv_k = time_step / jnp.where(joined, 2.0 * w_k, w_k)
    inv_x = [1.0 / v for v in weights]
    inv_y = [1.0 / v for v in weights]
    inv_x[0] = jnp.where(gx > 0, 0.5, 1.0) * inv_x[0]
    inv_x[7] = jnp.where(gx < nx - 1, 0.5, 1.0) * inv_x[7]
    inv_y[0] = jnp.where(gy > 0, 0.5, 1.0) * inv_y[0]
    inv_y[7] = jnp.where(gy < ny - 1, 0.5, 1.0) * inv_y[7]
    for i in range(8):
        for j in range(8):
            wm[i, 8 * j:8 * j + 8, :] = (weights[i] * weights[j]) * w_k
            dim[i, 8 * j:8 * j + 8, :] = (inv_x[i] * inv_y[j]) * inv_k

    part = 256
    for m in range(2):
        for b in range(half_rows // part):
            spot = slice(m * half_rows + b * part, m * half_rows + (b + 1) * part)
            to = slice(b * part, (b + 1) * part)
            point = point_ref[0:1, spot]
            eight = lax.broadcasted_iota(i32, (8, part), 0)
            tall = jnp.concatenate([eight + (64 * i + 8 * j) for i, j in FACE + INTERIOR], axis=0)
            short = lax.broadcasted_iota(i32, (ez, part), 0)
            spread_q[m, :, to] = jnp.where(tall == point // ez, 1.0, 0.0).astype(bf)
            spread_e[m, :, to] = jnp.where(short == lax.rem(point, ez), 1.0, 0.0).astype(bf)
        count = mm_t(spread_q[m], spread_e[m])
        for at, (i, j) in enumerate(FACE + INTERIOR):
            spot = slice(8 * j, 8 * j + 8)
            held[m, i, spot] = count[8 * at:8 * at + 8] * (penalty_rate * wm[i, spot])

    for load in loads:
        load.wait()

    def halo_copy(s, m, number):
        dx, dy = HEADINGS[number]
        lines = pl.ds(0 if dy < 0 else 56, 8)
        plane = 0 if dx < 0 else 7
        if dy == 0:
            source, target = local.at[m, plane], hx.at[s, number, m]
        elif dx == 0:
            source, target = local.at[m, :, lines, :], hy.at[s, number - 2, m]
        else:
            source, target = local.at[m, plane, lines, :], he.at[s, number - 4, m]
        return pltpu.make_async_remote_copy(
            src_ref=source, dst_ref=target, send_sem=halo_send.at[s, m, number], recv_sem=halo_recv.at[s, m, number],
            device_id=(gx + dx, gy + dy), device_id_type=MESH,
        )

    def inside(dx, dy):
        return (gx + dx >= 0) & (gx + dx < nx) & (gy + dy >= 0) & (gy + dy < ny)

    def operators(value):
        for m in range(2):
            lo = slice(m * ez, (m + 1) * ez)
            scale = nu_ref[m:m + 1, :]
            for half in range(2):
                some = slice(4 * half, 4 * half + 4)
                part = value[m, some].reshape(256, ez)
                grad[0, some, :, lo] = mm3(ops[0], ops[1], part).reshape(4, 64, ez)
                grad[1, some, :, lo] = mm3(ops[2], ops[3], part).reshape(4, 64, ez)
            for a in range(8):
                gxa = (2.0 * derivative[a][0]) * value[m, 0]
                for i in range(1, 8):
                    gxa = gxa + (2.0 * derivative[a][i]) * value[m, i]
                wma = wm[a]
                gya = grad[0, a, :, lo]
                gza = grad[1, a, :, lo]
                adv = vel[0, m, a] * gxa + vel[1, m, a] * gya + vel[2, m, a] * gza
                local[m, a] = -(wma * adv) - held[m, a] * value[m, a]
                wn = wma * scale
                work[m, a] = wn * gxa
                grad[0, a, :, lo] = wn * gya
                grad[1, a, :, lo] = wn * gza
            for half in range(2):
                some = slice(4 * half, 4 * half + 4)
                part_y = grad[0, some, :, lo].reshape(256, ez)
                part_z = grad[1, some, :, lo].reshape(256, ez)
                back = mm3(ops[4], ops[5], part_y) + mm3(ops[6], ops[7], part_z)
                local[m, some] -= back.reshape(4, 64, ez)
            for i in range(8):
                total = (2.0 * derivative[0][i]) * work[m, 0]
                for a in range(1, 8):
                    total = total + (2.0 * derivative[a][i]) * work[m, a]
                local[m, i] -= total

    operators(start)
    pltpu.make_async_copy(asked.at[me], got.at[me], in_sem.at[0]).start()
    pltpu.make_async_copy(asked.at[me], got.at[me], in_sem.at[0]).wait()
    def prepare(g):
        wanted = jnp.concatenate([got[g * per + t] for t in range(per)], axis=1)
        wide = lax.broadcasted_iota(i32, (2 * ez, lanes), 0)
        pick[g] = jnp.where(wide == wanted[3:4].astype(i32), 1.0, 0.0).astype(bf)
        away = [wanted - v for v in gll_nodes]
        before = [None, away[0]]
        for k in range(1, 7):
            before.append(before[-1] * away[k])
        after = [None] * 7 + [None]
        after[6] = away[7]
        for k in range(5, -1, -1):
            after[k] = after[k + 1] * away[k + 1]
        for j in range(8):
            norm = 1.0
            for k in range(8):
                if k != j:
                    norm *= gll_nodes[j] - gll_nodes[k]
            factor = after[0] if j == 0 else before[7] if j == 7 else before[j] * after[j]
            factor = factor * (1.0 / norm)
            for c in range(3):
                basis_ref[g, 8 * c + j:8 * c + j + 1, :] = factor[c:c + 1]

    def split_lines(value, lines, into):
        both = jnp.concatenate(
            [jnp.concatenate([value[m, i, 8 * j:8 * j + 8] for i, j in lines], axis=0) for m in range(2)], axis=1
        )
        lhs[0, into, :], lhs[1, into, :] = halves(both)

    face_at, inner_at = slice(0, 8 * len(FACE)), slice(8 * len(FACE), 512)

    def contract(lines, at_rows, g):
        found = mm(lhs[0, at_rows], pick[g]) + mm(lhs[1, at_rows], pick[g])
        total = None
        for j in range(8):
            line = None
            for at, (i, jj) in enumerate(lines):
                if jj == j:
                    term = found[8 * at:8 * at + 8] * basis_ref[g, i:i + 1, :]
                    line = term if line is None else line + term
            if line is not None:
                line = line * basis_ref[g, 8 + j:9 + j, :]
                total = line if total is None else total + line
        return total

    def sum_third(flat, m, first, size, stride):
        lane = lax.broadcasted_iota(i32, (size, ez), 1)
        low_rows, high_rows = pl.ds(first, size, stride=stride), pl.ds(first + 7, size, stride=stride)
        lower, upper = flat[m, low_rows, :], flat[m, high_rows, :]
        shared = upper + pltpu.roll(lower, ez - 1, 1)
        flat[m, high_rows, :] = jnp.where(lane < ez - 1, shared, upper)
        flat[m, low_rows, :] = jnp.where(lane > 0, pltpu.roll(shared, 1, 1), lower)

    flat = local.reshape(2, 512, ez)

    def halo_sent(s):
        for m in range(2):
            for number, (dx, dy) in enumerate(HEADINGS):
                @pl.when(inside(dx, dy))
                def _(m=m, number=number):
                    halo_copy(s, m, number).wait_send()

    for s in range(3):
        value = start if s == 0 else cur
        split_lines(value, FACE, face_at)

        def interpolate(g):
            if s == 0:
                total = contract(FACE + INTERIOR, slice(0, 512), g)
            else:
                total = contract(FACE, face_at, g) + inner_part[g]
            row = jnp.sum(total * basis_ref[g, 16:24, :], axis=0, keepdims=True)
            for t in range(per):
                ans[s, g * per + t] = row[:, t * cap:(t + 1) * cap]
            for t in range(per):
                d = g * per + t

                @pl.when(d != me)
                def _(d=d):
                    pltpu.make_async_remote_copy(
                        src_ref=ans.at[s, d], dst_ref=rep.at[s, me],
                        send_sem=ans_send.at[s], recv_sem=ans_recv.at[s],
                        device_id=place(d), device_id_type=MESH,
                    ).start()

        def from_afar(p, carry):
            off = groups // 2 + ((p + 1) // 2) * (1 - 2 * lax.rem(p, 2))
            interpolate(lax.rem(own_group + off + groups, groups))
            return carry

        def request(p, carry):
            off = ((p + 1) // 2) * (1 - 2 * lax.rem(p, 2))
            g = lax.rem(own_group + off + groups, groups)
            some = got.at[pl.ds(0, per)]
            pltpu.make_async_copy(some, some, ask_recv.at[g]).wait()
            prepare(g)
            return carry

        if s == 0:
            split_lines(value, INTERIOR, inner_at)
            nearby = got.at[pl.ds(0, per - 1)]
            pltpu.make_async_copy(nearby, nearby, ask_recv.at[own_group]).wait()
            prepare(own_group)
            early = 2

            def soon(p, carry):
                interpolate(lax.rem(own_group - p + groups, groups))
                return carry

            if early > 1:
                lax.fori_loop(1, early, request, 0)
            lax.fori_loop(0, early, soon, 0)
            lax.fori_loop(max(early, 1), groups, request, 0)
            lax.fori_loop(0, groups - early, from_afar, 0)
        else:
            lax.fori_loop(0, groups, from_afar, 0)
            halo_sent(s - 1)
        if s > 0:
            operators(cur)
        rep[s, me] = ans[s, me]
        arrived = ans.at[s, pl.ds(0, n - 1)]
        pltpu.make_async_copy(arrived, arrived, ans_recv.at[s]).wait()

        answers = jnp.concatenate([rep[s, d] for d in range(n)], axis=0)
        if cap < 128:
            answers = jnp.concatenate([answers, jnp.zeros((n, 128 - cap), f32)], axis=1)

        def scatter(m, lines, first):
            added = mm_t(spread_q[m, first:first + 8 * len(lines), :], spread_v[m])
            for at, (i, j) in enumerate(lines):
                spot, rows_at = slice(8 * j, 8 * j + 8), slice(8 * at, 8 * at + 8)
                local[m, i, spot] += (penalty_rate * wm[i, spot]) * (added[rows_at, :ez] + added[rows_at, ez:])

        spread_v = []
        for m in range(2):
            pieces = []
            for t in range(half_rows // 128):
                spot = slice(m * half_rows + t * 128, m * half_rows + (t + 1) * 128)
                slot = jnp.broadcast_to(rank_s[0:1, spot], (n, 128))
                taken = jnp.take_along_axis(answers, slot, axis=1)
                own = owner_ref[0:1, spot] == lax.broadcasted_iota(i32, (n, 128), 0)
                pieces.append(jnp.sum(jnp.where(own, taken, 0.0), axis=0, keepdims=True))
            row_high, row_low = halves(jnp.concatenate(pieces, axis=1))
            where_e = spread_e[m]
            spread_v.append(jnp.concatenate([where_e * row_high, where_e * row_low], axis=0))
            scatter(m, FACE, 0)
            for i in (0, 7):
                sum_third(flat, m, 64 * i + 8, 6, 8)
            for j in (0, 7):
                sum_third(flat, m, 8 * j, 8, 64)
            for number, (dx, dy) in enumerate(HEADINGS):
                @pl.when(inside(dx, dy))
                def _(m=m, number=number):
                    halo_copy(s, m, number).start()

        target = cur if s < 2 else out_ref
        share = (1.0, 0.25, 2.0 / 3.0)[s]
        for m in range(2):
            scatter(m, INTERIOR, 8 * len(FACE))
            for i in INNER:
                sum_third(flat, m, 64 * i + 8, 6, 8)
            for i in range(8):
                moved = value[m, i] + local[m, i] * dim[i]
                if s == 0:
                    cur[m, i] = moved
                elif s == 1:
                    cur[m, i] = 0.75 * start[m, i] + 0.25 * moved
                else:
                    out_ref[m, i] = start[m, i] * (1.0 / 3.0) + (2.0 / 3.0) * moved
        if s < 2:
            split_lines(cur, INTERIOR, inner_at)

            def ahead(g, carry):
                inner_part[g] = contract(INTERIOR, inner_at, g)
                return carry

            lax.fori_loop(0, groups, ahead, 0)
        for m in range(2):
            for number, (dx, dy) in enumerate(HEADINGS):
                @pl.when(inside(-dx, -dy))
                def _(m=m, number=number, dx=dx, dy=dy):
                    halo_copy(s, m, number).wait_recv()
                    plane = 7 if dx < 0 else 0
                    lines = slice(56, 64) if dy < 0 else slice(0, 8)
                    if dy == 0:
                        target[m, plane] += hx[s, number, m] * (share * dim[plane])
                    elif dx == 0:
                        target[m, :, lines, :] += hy[s, number - 2, m] * (share * dim[:, lines, :])
                    else:
                        target[m, plane, lines, :] += he[s, number - 4, m] * (share * dim[plane, lines, :])
    halo_sent(2)
    sent = got.at[pl.ds(0, n - 1)]
    pltpu.make_async_copy(sent, sent, ask_send).wait()
    for s in range(3):
        whole = ans.at[s, pl.ds(0, n - 1)]
        pltpu.make_async_copy(whole, whole, ans_send.at[s]).wait()


def split_host(matrix):
    high = matrix.astype(jnp.bfloat16)
    low = (matrix - high.astype(np.float64)).astype(jnp.bfloat16)
    return [high, low]


def body(scalar, velocity, diffusivity, recv_owner, donor_elem, recv_point, recv_coords):
    tables = gll_tables()
    derivative = tables[2]
    ez = scalar.shape[4]
    n = lax.axis_size("gx") * lax.axis_size("gy")
    rows = recv_owner.shape[0]
    cap = max(2, 2 * rows // n)
    per = max(1, min(n, 512 // cap))
    groups, lanes = n // per, per * cap
    width = min(256, rows)
    blocks = rows // width
    bf, f32, i32 = jnp.bfloat16, jnp.float32, jnp.int32

    half_eye = np.eye(4)
    table = 2.0 * np.asarray(derivative, np.float64)
    along_y = np.kron(half_eye, np.kron(table, np.eye(8)))
    along_z = np.kron(half_eye, np.kron(np.eye(8), table))
    ops = []
    for matrix in (along_y, along_z, along_y.T, along_z.T):
        ops = ops + split_host(matrix)
    ops = jnp.asarray(np.stack(ops))

    vmem = pltpu.VMEM
    dma = pltpu.SemaphoreType.DMA
    field = (2, 8, 64, ez)
    in_vmem, anywhere = pl.BlockSpec(memory_space=vmem), pl.BlockSpec(memory_space=pltpu.HBM)
    out = pl.pallas_call(
        functools.partial(step_kernel, tables),
        out_shape=jax.ShapeDtypeStruct(field, f32),
        in_specs=[in_vmem] * 5 + [anywhere] * 3,
        out_specs=in_vmem,
        scratch_shapes=[
            vmem(field, f32),
            vmem((3,) + field, f32),
            vmem((8, 256, 256), bf),
            vmem(field, f32),
            vmem(field, f32),
            vmem(field, f32),
            vmem((2, 8, 64, 2 * ez), f32),
            vmem((8, 64, ez), f32),
            vmem((8, 64, ez), f32),
            vmem(field, f32),
            vmem((blocks * n, width), bf),
            vmem((blocks * n, width), f32),
            vmem((1, rows), i32),
            vmem((n, 4, cap), f32),
            vmem((n, 4, cap), f32),
            vmem((groups, 2 * ez, lanes), bf),
            vmem((groups, 24, lanes), f32),
            vmem((2, 512, rows // 2), bf),
            vmem((2, ez, rows // 2), bf),
            vmem((3, n, 1, cap), f32),
            vmem((3, n, 1, cap), f32),
            vmem((3, 2, 2, 64, ez), f32),
            vmem((3, 2, 2, 8, 8, ez), f32),
            vmem((3, 4, 2, 8, ez), f32),
            vmem((2, 512, 2 * ez), bf),
            vmem((groups, 8, lanes), f32),
            dma((3,)),
            dma,
            dma((groups,)),
            dma((3,)),
            dma((3,)),
            dma((3, 2, 8)),
            dma((3, 2, 8)),
        ],
        compiler_params=pltpu.CompilerParams(collective_id=0, has_side_effects=True, vmem_limit_bytes=44 * 1024 * 1024),
        name="advance",
    )(
        *[pltpu.with_memory_space_constraint(v, pltpu.HBM) for v in (
            recv_owner.reshape(1, rows), donor_elem.reshape(1, rows), recv_point.reshape(1, rows), recv_coords,
            diffusivity.reshape(2, ez), scalar.reshape(field), velocity.reshape((3,) + field), ops,
        )]
    )
    return out.reshape(scalar.shape)


def solution(mesh):
    return jax.shard_map(
        body,
        mesh=mesh,
        in_specs=(
            P(None, None, "gx", "gy", None),
            P(None, None, None, "gx", "gy", None),
            P(None, "gx", "gy", None),
            P(("gx", "gy"), None),
            P(("gx", "gy")),
            P(("gx", "gy")),
            P(None, ("gx", "gy")),
        ),
        out_specs=P(None, None, "gx", "gy", None),
        check_vma=False,
    )
```

```python
import functools
import jax
import jax.numpy as jnp
import numpy as np
from jax import lax
from jax.experimental import pallas as pl
from jax.experimental.pallas import tpu as pltpu
from jax.sharding import PartitionSpec as P

time_step = 0.01
penalty_rate = 50.0
volume_factor = 0.125
node_inner = [0.8717401485096066, 0.5917001814331423, 0.20929921790247888]


def legendre_seven(point):
    before, current = (1.0, point)
    for order in range(1, 7):
        before, current = (
            current,
            ((2 * order + 1) * point * current - order * before) / (order + 1),
        )
    return current


def gll_tables():
    degree = 7
    gll_nodes = [-1.0] + [-v for v in node_inner] + node_inner[::-1] + [1.0]
    end_values = [legendre_seven(v) for v in gll_nodes]
    weights = [2.0 / (degree * (degree + 1) * v * v) for v in end_values]
    derivative = [[0.0] * 8 for _ in range(8)]
    for a in range(8):
        for b in range(8):
            if a != b:
                derivative[a][b] = end_values[a] / (end_values[b] * (gll_nodes[a] - gll_nodes[b]))
    derivative[0][0] = -degree * (degree + 1) / 4.0
    derivative[7][7] = degree * (degree + 1) / 4.0
    return (gll_nodes, weights, derivative)


MESH = pl.DeviceIdType.MESH
HEADINGS = [(-1, 0), (1, 0), (0, -1), (0, 1), (-1, -1), (-1, 1), (1, -1), (1, 1)]
INNER = range(1, 7)
FACE = [(i, j) for i in (0, 7) for j in range(8)] + [(i, j) for j in (0, 7) for i in INNER]
INTERIOR = [(i, j) for i in INNER for j in INNER]


def halves(value):
    high = value.astype(jnp.bfloat16)
    return high, (value - high.astype(jnp.float32)).astype(jnp.bfloat16)


def mm(a, b):
    return jnp.dot(a, b, preferred_element_type=jnp.float32)


def mm_t(a, b):
    return lax.dot_general(a, b, (((1,), (1,)), ((), ())), preferred_element_type=jnp.float32)


def mm3(op_high, op_low, value):
    high, low = halves(value)
    return mm(op_high, high) + mm(op_high, low) + mm(op_low, high)


def step_kernel(
    tables, owner_ref, elem_ref, point_ref, coord_ref, nu_ref, start_hbm, vel_hbm, ops_hbm,
    out_ref,
    start, vel, ops, cur, local, work, grad, wm, dim, held,
    hot_s, within_s, rank_s, asked, got, pick, basis_ref, spread_q, spread_e,
    ans, rep, hx, hy, he, lhs, inner_part,
    in_sem, ask_send, ask_recv, ans_send, ans_recv, halo_send, halo_recv,
):
    gll_nodes, weights, derivative = tables
    f32, bf, i32 = jnp.float32, jnp.bfloat16, jnp.int32
    gx, gy = lax.axis_index("gx"), lax.axis_index("gy")
    nx, ny = lax.axis_size("gx"), lax.axis_size("gy")
    n = nx * ny
    me = gx * ny + gy
    ez = start.shape[-1]
    rows = owner_ref.shape[-1]
    cap = ans.shape[-1]
    groups, _, lanes = pick.shape
    per = lanes // cap
    width = within_s.shape[-1]
    blocks = rows // width
    half_rows = rows // 2

    barrier = pltpu.get_barrier_semaphore()

    def place(d):
        return (d // ny, lax.rem(d, ny))

    def greet(a, carry):
        px = lax.rem(gx + nx // 2 + a, nx)
        for b in range(ny):
            @pl.when((px != gx) | (gy != b))
            def _(b=b):
                pl.semaphore_signal(barrier, inc=1, device_id=(px, b), device_id_type=MESH)

        return carry

    lax.fori_loop(0, nx, greet, 0)
    loads = [
        pltpu.make_async_copy(start_hbm, start, in_sem.at[0]),
        pltpu.make_async_copy(vel_hbm, vel, in_sem.at[1]),
        pltpu.make_async_copy(ops_hbm, ops, in_sem.at[2]),
    ]
    for load in loads:
        load.start()

    for b in range(blocks):
        spot = slice(b * width, (b + 1) * width)
        iota_n = lax.broadcasted_iota(i32, (n, width), 0)
        hot_s[b * n:(b + 1) * n, :] = jnp.where(owner_ref[0:1, spot] == iota_n, 1.0, 0.0).astype(bf)
    first_of = lax.broadcasted_iota(i32, (width, width), 0)
    second_of = lax.broadcasted_iota(i32, (width, width), 1)
    earlier = jnp.where(first_of < second_of, 1.0, 0.0).astype(bf)
    within_s[...] = mm(hot_s[...], earlier)
    sums = mm(hot_s[...], jnp.ones((width, 128), bf))
    offset = jnp.zeros((n, 128), f32)
    inverse = jnp.zeros((2 * n, 128), f32)
    lane_f = lax.broadcasted_iota(i32, (n, width), 1).astype(f32)
    slot_iota = lax.broadcasted_iota(i32, (128, width), 0)
    for b in range(blocks):
        spot = slice(b * width, (b + 1) * width)
        mine = hot_s[b * n:(b + 1) * n, :].astype(f32)
        wide_offset = jnp.concatenate([offset] * (width // 128), axis=1)
        place_in = (within_s[b * n:(b + 1) * n, :] + wide_offset) * mine
        rank = jnp.sum(place_in, axis=0, keepdims=True).astype(i32)
        rank_s[0:1, spot] = rank
        slot_hot = jnp.where(slot_iota == rank, 1.0, 0.0).astype(bf)
        named = jnp.concatenate([mine * lane_f, mine * float(b)], axis=0).astype(bf)
        inverse = inverse + mm_t(named, slot_hot)
        offset = offset + sums[b * n:(b + 1) * n, :]
    source = (inverse[0:n] + float(width) * inverse[n:2 * n]).astype(i32)
    tile_of, lane_of = source // 128, lax.rem(source, 128)
    found = [jnp.zeros((n, 128), f32) for _ in range(4)]
    for t in range(rows // 128):
        spot = slice(t * 128, (t + 1) * 128)
        here = tile_of == t
        for c in range(4):
            row = coord_ref[c:c + 1, spot] if c < 3 else elem_ref[0:1, spot].astype(f32)
            picked = jnp.take_along_axis(jnp.broadcast_to(row, (n, 128)), lane_of, axis=1)
            found[c] = jnp.where(here, picked, found[c])
    found[3] = found[3] + jnp.where(source < half_rows, float(ez), 0.0)
    for c in range(4):
        for d in range(n):
            asked[d, c:c + 1, :] = found[c][d:d + 1, 0:cap]

    pl.semaphore_wait(barrier, n - 1)

    own_group = me // per

    def ask(a, carry):
        px = lax.rem(gx + nx // 2 + a, nx)
        for b in range(ny):
            @pl.when((px != gx) | (gy != b))
            def _(b=b):
                pltpu.make_async_remote_copy(
                    src_ref=asked.at[px * ny + b], dst_ref=got.at[me],
                    send_sem=ask_send, recv_sem=ask_recv.at[own_group],
                    device_id=(px, b), device_id_type=MESH,
                ).start()

        return carry

    lax.fori_loop(0, nx, ask, 0)

    k_iota = lax.broadcasted_iota(i32, (8, ez), 0)
    e_iota = lax.broadcasted_iota(i32, (8, ez), 1)
    w_k = jnp.zeros((8, ez), f32)
    for k in range(8):
        w_k = jnp.where(k_iota == k, volume_factor * weights[k], w_k)
    joined = ((k_iota == 0) & (e_iota > 0)) | ((k_iota == 7) & (e_iota < ez - 1))
    inv_k = time_step / jnp.where(joined, 2.0 * w_k, w_k)
    inv_x = [1.0 / v for v in weights]
    inv_y = [1.0 / v for v in weights]
    inv_x[0] = jnp.where(gx > 0, 0.5, 1.0) * inv_x[0]
    inv_x[7] = jnp.where(gx < nx - 1, 0.5, 1.0) * inv_x[7]
    inv_y[0] = jnp.where(gy > 0, 0.5, 1.0) * inv_y[0]
    inv_y[7] = jnp.where(gy < ny - 1, 0.5, 1.0) * inv_y[7]
    for i in range(8):
        for j in range(8):
            wm[i, 8 * j:8 * j + 8, :] = (weights[i] * weights[j]) * w_k
            dim[i, 8 * j:8 * j + 8, :] = (inv_x[i] * inv_y[j]) * inv_k

    part = 256
    for m in range(2):
        for b in range(half_rows // part):
            spot = slice(m * half_rows + b * part, m * half_rows + (b + 1) * part)
            to = slice(b * part, (b + 1) * part)
            point = point_ref[0:1, spot]
            eight = lax.broadcasted_iota(i32, (8, part), 0)
            tall = jnp.concatenate([eight + (64 * i + 8 * j) for i, j in FACE + INTERIOR], axis=0)
            short = lax.broadcasted_iota(i32, (ez, part), 0)
            spread_q[m, :, to] = jnp.where(tall == point // ez, 1.0, 0.0).astype(bf)
            spread_e[m, :, to] = jnp.where(short == lax.rem(point, ez), 1.0, 0.0).astype(bf)
        count = mm_t(spread_q[m], spread_e[m])
        for at, (i, j) in enumerate(FACE + INTERIOR):
            spot = slice(8 * j, 8 * j + 8)
            held[m, i, spot] = count[8 * at:8 * at + 8] * (penalty_rate * wm[i, spot])

    for load in loads:
        load.wait()

    def halo_copy(s, m, number):
        dx, dy = HEADINGS[number]
        lines = pl.ds(0 if dy < 0 else 56, 8)
        plane = 0 if dx < 0 else 7
        if dy == 0:
            source, target = local.at[m, plane], hx.at[s, number, m]
        elif dx == 0:
            source, target = local.at[m, :, lines, :], hy.at[s, number - 2, m]
        else:
            source, target = local.at[m, plane, lines, :], he.at[s, number - 4, m]
        return pltpu.make_async_remote_copy(
            src_ref=source, dst_ref=target, send_sem=halo_send.at[s, m, number], recv_sem=halo_recv.at[s, m, number],
            device_id=(gx + dx, gy + dy), device_id_type=MESH,
        )

    def inside(dx, dy):
        return (gx + dx >= 0) & (gx + dx < nx) & (gy + dy >= 0) & (gy + dy < ny)

    def operators(value):
        for m in range(2):
            lo = slice(m * ez, (m + 1) * ez)
            scale = nu_ref[m:m + 1, :]
            for half in range(2):
                some = slice(4 * half, 4 * half + 4)
                part = value[m, some].reshape(256, ez)
                grad[0, some, :, lo] = mm3(ops[0], ops[1], part).reshape(4, 64, ez)
                grad[1, some, :, lo] = mm3(ops[2], ops[3], part).reshape(4, 64, ez)
            for a in range(8):
                gxa = (2.0 * derivative[a][0]) * value[m, 0]
                for i in range(1, 8):
                    gxa = gxa + (2.0 * derivative[a][i]) * value[m, i]
                wma = wm[a]
                gya = grad[0, a, :, lo]
                gza = grad[1, a, :, lo]
                adv = vel[0, m, a] * gxa + vel[1, m, a] * gya + vel[2, m, a] * gza
                local[m, a] = -(wma * adv) - held[m, a] * value[m, a]
                wn = wma * scale
                work[m, a] = wn * gxa
                grad[0, a, :, lo] = wn * gya
                grad[1, a, :, lo] = wn * gza
            for half in range(2):
                some = slice(4 * half, 4 * half + 4)
                part_y = grad[0, some, :, lo].reshape(256, ez)
                part_z = grad[1, some, :, lo].reshape(256, ez)
                back = mm3(ops[4], ops[5], part_y) + mm3(ops[6], ops[7], part_z)
                local[m, some] -= back.reshape(4, 64, ez)
            for i in range(8):
                total = (2.0 * derivative[0][i]) * work[m, 0]
                for a in range(1, 8):
                    total = total + (2.0 * derivative[a][i]) * work[m, a]
                local[m, i] -= total

    operators(start)
    pltpu.make_async_copy(asked.at[me], got.at[me], in_sem.at[0]).start()
    pltpu.make_async_copy(asked.at[me], got.at[me], in_sem.at[0]).wait()
    def prepare(g):
        wanted = jnp.concatenate([got[g * per + t] for t in range(per)], axis=1)
        wide = lax.broadcasted_iota(i32, (2 * ez, lanes), 0)
        pick[g] = jnp.where(wide == wanted[3:4].astype(i32), 1.0, 0.0).astype(bf)
        away = [wanted - v for v in gll_nodes]
        before = [None, away[0]]
        for k in range(1, 7):
            before.append(before[-1] * away[k])
        after = [None] * 7 + [None]
        after[6] = away[7]
        for k in range(5, -1, -1):
            after[k] = after[k + 1] * away[k + 1]
        for j in range(8):
            norm = 1.0
            for k in range(8):
                if k != j:
                    norm *= gll_nodes[j] - gll_nodes[k]
            factor = after[0] if j == 0 else before[7] if j == 7 else before[j] * after[j]
            factor = factor * (1.0 / norm)
            for c in range(3):
                basis_ref[g, 8 * c + j:8 * c + j + 1, :] = factor[c:c + 1]

    def split_lines(value, lines, into):
        both = jnp.concatenate(
            [jnp.concatenate([value[m, i, 8 * j:8 * j + 8] for i, j in lines], axis=0) for m in range(2)], axis=1
        )
        lhs[0, into, :], lhs[1, into, :] = halves(both)

    face_at, inner_at = slice(0, 8 * len(FACE)), slice(8 * len(FACE), 512)

    def contract(lines, at_rows, g):
        found = mm(lhs[0, at_rows], pick[g]) + mm(lhs[1, at_rows], pick[g])
        total = None
        for j in range(8):
            line = None
            for at, (i, jj) in enumerate(lines):
                if jj == j:
                    term = found[8 * at:8 * at + 8] * basis_ref[g, i:i + 1, :]
                    line = term if line is None else line + term
            if line is not None:
                line = line * basis_ref[g, 8 + j:9 + j, :]
                total = line if total is None else total + line
        return total

    def sum_third(flat, m, first, size, stride):
        lane = lax.broadcasted_iota(i32, (size, ez), 1)
        low_rows, high_rows = pl.ds(first, size, stride=stride), pl.ds(first + 7, size, stride=stride)
        lower, upper = flat[m, low_rows, :], flat[m, high_rows, :]
        shared = upper + pltpu.roll(lower, ez - 1, 1)
        flat[m, high_rows, :] = jnp.where(lane < ez - 1, shared, upper)
        flat[m, low_rows, :] = jnp.where(lane > 0, pltpu.roll(shared, 1, 1), lower)

    flat = local.reshape(2, 512, ez)

    def halo_sent(s):
        for m in range(2):
            for number, (dx, dy) in enumerate(HEADINGS):
                @pl.when(inside(dx, dy))
                def _(m=m, number=number):
                    halo_copy(s, m, number).wait_send()

    for s in range(3):
        value = start if s == 0 else cur
        split_lines(value, FACE, face_at)

        def interpolate(g):
            if s == 0:
                total = contract(FACE + INTERIOR, slice(0, 512), g)
            else:
                total = contract(FACE, face_at, g) + inner_part[g]
            row = jnp.sum(total * basis_ref[g, 16:24, :], axis=0, keepdims=True)
            for t in range(per):
                ans[s, g * per + t] = row[:, t * cap:(t + 1) * cap]
            for t in range(per):
                d = g * per + t

                @pl.when(d != me)
                def _(d=d):
                    pltpu.make_async_remote_copy(
                        src_ref=ans.at[s, d], dst_ref=rep.at[s, me],
                        send_sem=ans_send.at[s], recv_sem=ans_recv.at[s],
                        device_id=place(d), device_id_type=MESH,
                    ).start()

        def from_afar(p, carry):
            off = groups // 2 + ((p + 1) // 2) * (1 - 2 * lax.rem(p, 2))
            interpolate(lax.rem(own_group + off + groups, groups))
            return carry

        def request(p, carry):
            off = ((p + 1) // 2) * (1 - 2 * lax.rem(p, 2))
            g = lax.rem(own_group + off + groups, groups)
            some = got.at[pl.ds(0, per)]
            pltpu.make_async_copy(some, some, ask_recv.at[g]).wait()
            prepare(g)
            return carry

        if s == 0:
            split_lines(value, INTERIOR, inner_at)
            nearby = got.at[pl.ds(0, per - 1)]
            pltpu.make_async_copy(nearby, nearby, ask_recv.at[own_group]).wait()
            prepare(own_group)
            early = 2

            def soon(p, carry):
                interpolate(lax.rem(own_group - p + groups, groups))
                return carry

            if early > 1:
                lax.fori_loop(1, early, request, 0)
            lax.fori_loop(0, early, soon, 0)
            lax.fori_loop(max(early, 1), groups, request, 0)
            lax.fori_loop(0, groups - early, from_afar, 0)
        else:
            lax.fori_loop(0, groups, from_afar, 0, unroll=2)
            halo_sent(s - 1)
        if s > 0:
            operators(cur)
        rep[s, me] = ans[s, me]
        arrived = ans.at[s, pl.ds(0, n - 1)]
        pltpu.make_async_copy(arrived, arrived, ans_recv.at[s]).wait()

        answers = jnp.concatenate([rep[s, d] for d in range(n)], axis=0)
        if cap < 128:
            answers = jnp.concatenate([answers, jnp.zeros((n, 128 - cap), f32)], axis=1)

        def scatter(m, lines, first):
            added = mm_t(spread_q[m, first:first + 8 * len(lines), :], spread_v[m])
            for at, (i, j) in enumerate(lines):
                spot, rows_at = slice(8 * j, 8 * j + 8), slice(8 * at, 8 * at + 8)
                local[m, i, spot] += (penalty_rate * wm[i, spot]) * (added[rows_at, :ez] + added[rows_at, ez:])

        spread_v = []
        for m in range(2):
            pieces = []
            for t in range(half_rows // 128):
                spot = slice(m * half_rows + t * 128, m * half_rows + (t + 1) * 128)
                slot = jnp.broadcast_to(rank_s[0:1, spot], (n, 128))
                taken = jnp.take_along_axis(answers, slot, axis=1)
                own = owner_ref[0:1, spot] == lax.broadcasted_iota(i32, (n, 128), 0)
                pieces.append(jnp.sum(jnp.where(own, taken, 0.0), axis=0, keepdims=True))
            row_high, row_low = halves(jnp.concatenate(pieces, axis=1))
            where_e = spread_e[m]
            spread_v.append(jnp.concatenate([where_e * row_high, where_e * row_low], axis=0))
            scatter(m, FACE, 0)
            for i in (0, 7):
                sum_third(flat, m, 64 * i + 8, 6, 8)
            for j in (0, 7):
                sum_third(flat, m, 8 * j, 8, 64)
            for number, (dx, dy) in enumerate(HEADINGS):
                @pl.when(inside(dx, dy))
                def _(m=m, number=number):
                    halo_copy(s, m, number).start()

        target = cur if s < 2 else out_ref
        share = (1.0, 0.25, 2.0 / 3.0)[s]
        for m in range(2):
            scatter(m, INTERIOR, 8 * len(FACE))
            for i in INNER:
                sum_third(flat, m, 64 * i + 8, 6, 8)
            for i in range(8):
                moved = value[m, i] + local[m, i] * dim[i]
                if s == 0:
                    cur[m, i] = moved
                elif s == 1:
                    cur[m, i] = 0.75 * start[m, i] + 0.25 * moved
                else:
                    out_ref[m, i] = start[m, i] * (1.0 / 3.0) + (2.0 / 3.0) * moved
        if s < 2:
            split_lines(cur, INTERIOR, inner_at)

            def ahead(g, carry):
                inner_part[g] = contract(INTERIOR, inner_at, g)
                return carry

            lax.fori_loop(0, groups, ahead, 0, unroll=2)
        for m in range(2):
            for number, (dx, dy) in enumerate(HEADINGS):
                @pl.when(inside(-dx, -dy))
                def _(m=m, number=number, dx=dx, dy=dy):
                    halo_copy(s, m, number).wait_recv()
                    plane = 7 if dx < 0 else 0
                    lines = slice(56, 64) if dy < 0 else slice(0, 8)
                    if dy == 0:
                        target[m, plane] += hx[s, number, m] * (share * dim[plane])
                    elif dx == 0:
                        target[m, :, lines, :] += hy[s, number - 2, m] * (share * dim[:, lines, :])
                    else:
                        target[m, plane, lines, :] += he[s, number - 4, m] * (share * dim[plane, lines, :])
    halo_sent(2)
    sent = got.at[pl.ds(0, n - 1)]
    pltpu.make_async_copy(sent, sent, ask_send).wait()
    for s in range(3):
        whole = ans.at[s, pl.ds(0, n - 1)]
        pltpu.make_async_copy(whole, whole, ans_send.at[s]).wait()


def split_host(matrix):
    high = matrix.astype(jnp.bfloat16)
    low = (matrix - high.astype(np.float64)).astype(jnp.bfloat16)
    return [high, low]


def body(scalar, velocity, diffusivity, recv_owner, donor_elem, recv_point, recv_coords):
    tables = gll_tables()
    derivative = tables[2]
    ez = scalar.shape[4]
    n = lax.axis_size("gx") * lax.axis_size("gy")
    rows = recv_owner.shape[0]
    cap = max(2, 2 * rows // n)
    per = max(1, min(n, 512 // cap))
    groups, lanes = n // per, per * cap
    width = min(256, rows)
    blocks = rows // width
    bf, f32, i32 = jnp.bfloat16, jnp.float32, jnp.int32

    half_eye = np.eye(4)
    table = 2.0 * np.asarray(derivative, np.float64)
    along_y = np.kron(half_eye, np.kron(table, np.eye(8)))
    along_z = np.kron(half_eye, np.kron(np.eye(8), table))
    ops = []
    for matrix in (along_y, along_z, along_y.T, along_z.T):
        ops = ops + split_host(matrix)
    ops = jnp.asarray(np.stack(ops))

    vmem = pltpu.VMEM
    dma = pltpu.SemaphoreType.DMA
    field = (2, 8, 64, ez)
    in_vmem, anywhere = pl.BlockSpec(memory_space=vmem), pl.BlockSpec(memory_space=pltpu.HBM)
    out = pl.pallas_call(
        functools.partial(step_kernel, tables),
        out_shape=jax.ShapeDtypeStruct(field, f32),
        in_specs=[in_vmem] * 5 + [anywhere] * 3,
        out_specs=in_vmem,
        scratch_shapes=[
            vmem(field, f32),
            vmem((3,) + field, f32),
            vmem((8, 256, 256), bf),
            vmem(field, f32),
            vmem(field, f32),
            vmem(field, f32),
            vmem((2, 8, 64, 2 * ez), f32),
            vmem((8, 64, ez), f32),
            vmem((8, 64, ez), f32),
            vmem(field, f32),
            vmem((blocks * n, width), bf),
            vmem((blocks * n, width), f32),
            vmem((1, rows), i32),
            vmem((n, 4, cap), f32),
            vmem((n, 4, cap), f32),
            vmem((groups, 2 * ez, lanes), bf),
            vmem((groups, 24, lanes), f32),
            vmem((2, 512, rows // 2), bf),
            vmem((2, ez, rows // 2), bf),
            vmem((3, n, 1, cap), f32),
            vmem((3, n, 1, cap), f32),
            vmem((3, 2, 2, 64, ez), f32),
            vmem((3, 2, 2, 8, 8, ez), f32),
            vmem((3, 4, 2, 8, ez), f32),
            vmem((2, 512, 2 * ez), bf),
            vmem((groups, 8, lanes), f32),
            dma((3,)),
            dma,
            dma((groups,)),
            dma((3,)),
            dma((3,)),
            dma((3, 2, 8)),
            dma((3, 2, 8)),
        ],
        compiler_params=pltpu.CompilerParams(collective_id=0, has_side_effects=True, vmem_limit_bytes=44 * 1024 * 1024),
        name="advance",
    )(
        *[pltpu.with_memory_space_constraint(v, pltpu.HBM) for v in (
            recv_owner.reshape(1, rows), donor_elem.reshape(1, rows), recv_point.reshape(1, rows), recv_coords,
            diffusivity.reshape(2, ez), scalar.reshape(field), velocity.reshape((3,) + field), ops,
        )]
    )
    return out.reshape(scalar.shape)


def solution(mesh):
    return jax.shard_map(
        body,
        mesh=mesh,
        in_specs=(
            P(None, None, "gx", "gy", None),
            P(None, None, None, "gx", "gy", None),
            P(None, "gx", "gy", None),
            P(("gx", "gy"), None),
            P(("gx", "gy")),
            P(("gx", "gy")),
            P(None, ("gx", "gy")),
        ),
        out_specs=P(None, None, "gx", "gy", None),
        check_vma=False,
    )
```

```python
import functools
import jax
import jax.numpy as jnp
import numpy as np
from jax import lax
from jax.experimental import pallas as pl
from jax.experimental.pallas import tpu as pltpu
from jax.sharding import PartitionSpec as P

time_step = 0.01
penalty_rate = 50.0
volume_factor = 0.125
node_inner = [0.8717401485096066, 0.5917001814331423, 0.20929921790247888]


def legendre_seven(point):
    before, current = (1.0, point)
    for order in range(1, 7):
        before, current = (
            current,
            ((2 * order + 1) * point * current - order * before) / (order + 1),
        )
    return current


def gll_tables():
    degree = 7
    gll_nodes = [-1.0] + [-v for v in node_inner] + node_inner[::-1] + [1.0]
    end_values = [legendre_seven(v) for v in gll_nodes]
    weights = [2.0 / (degree * (degree + 1) * v * v) for v in end_values]
    derivative = [[0.0] * 8 for _ in range(8)]
    for a in range(8):
        for b in range(8):
            if a != b:
                derivative[a][b] = end_values[a] / (end_values[b] * (gll_nodes[a] - gll_nodes[b]))
    derivative[0][0] = -degree * (degree + 1) / 4.0
    derivative[7][7] = degree * (degree + 1) / 4.0
    return (gll_nodes, weights, derivative)


MESH = pl.DeviceIdType.MESH
HEADINGS = [(-1, 0), (1, 0), (0, -1), (0, 1), (-1, -1), (-1, 1), (1, -1), (1, 1)]
INNER = range(1, 7)
FACE = [(i, j) for i in (0, 7) for j in range(8)] + [(i, j) for j in (0, 7) for i in INNER]
INTERIOR = [(i, j) for i in INNER for j in INNER]


def halves(value):
    high = value.astype(jnp.bfloat16)
    return high, (value - high.astype(jnp.float32)).astype(jnp.bfloat16)


def mm(a, b):
    return jnp.dot(a, b, preferred_element_type=jnp.float32)


def mm_t(a, b):
    return lax.dot_general(a, b, (((1,), (1,)), ((), ())), preferred_element_type=jnp.float32)


def mm3(op_high, op_low, value):
    high, low = halves(value)
    return mm(op_high, high) + mm(op_high, low) + mm(op_low, high)


def step_kernel(
    tables, owner_ref, elem_ref, point_ref, coord_ref, nu_ref, start_hbm, vel_hbm, ops_hbm,
    out_ref,
    start, vel, ops, cur, local, work, grad, wm, dim, held,
    hot_s, within_s, rank_s, asked, got, pick, basis_ref, spread_q, spread_e,
    ans, rep, hx, hy, he, lhs, inner_part,
    in_sem, ask_send, ask_recv, ans_send, ans_recv, halo_send, halo_recv,
):
    gll_nodes, weights, derivative = tables
    f32, bf, i32 = jnp.float32, jnp.bfloat16, jnp.int32
    gx, gy = lax.axis_index("gx"), lax.axis_index("gy")
    nx, ny = lax.axis_size("gx"), lax.axis_size("gy")
    n = nx * ny
    me = gx * ny + gy
    ez = start.shape[-1]
    rows = owner_ref.shape[-1]
    cap = ans.shape[-1]
    groups, _, lanes = pick.shape
    per = lanes // cap
    width = within_s.shape[-1]
    blocks = rows // width
    half_rows = rows // 2

    barrier = pltpu.get_barrier_semaphore()

    def place(d):
        return (d // ny, lax.rem(d, ny))

    def greet(a, carry):
        px = lax.rem(gx + nx // 2 + a, nx)
        for b in range(ny):
            @pl.when((px != gx) | (gy != b))
            def _(b=b):
                pl.semaphore_signal(barrier, inc=1, device_id=(px, b), device_id_type=MESH)

        return carry

    lax.fori_loop(0, nx, greet, 0)
    loads = [
        pltpu.make_async_copy(start_hbm, start, in_sem.at[0]),
        pltpu.make_async_copy(vel_hbm, vel, in_sem.at[1]),
        pltpu.make_async_copy(ops_hbm, ops, in_sem.at[2]),
    ]
    for load in loads:
        load.start()

    for b in range(blocks):
        spot = slice(b * width, (b + 1) * width)
        iota_n = lax.broadcasted_iota(i32, (n, width), 0)
        hot_s[b * n:(b + 1) * n, :] = jnp.where(owner_ref[0:1, spot] == iota_n, 1.0, 0.0).astype(bf)
    first_of = lax.broadcasted_iota(i32, (width, width), 0)
    second_of = lax.broadcasted_iota(i32, (width, width), 1)
    earlier = jnp.where(first_of < second_of, 1.0, 0.0).astype(bf)
    within_s[...] = mm(hot_s[...], earlier)
    sums = mm(hot_s[...], jnp.ones((width, 128), bf))
    offset = jnp.zeros((n, 128), f32)
    inverse = jnp.zeros((2 * n, 128), f32)
    lane_f = lax.broadcasted_iota(i32, (n, width), 1).astype(f32)
    slot_iota = lax.broadcasted_iota(i32, (128, width), 0)
    for b in range(blocks):
        spot = slice(b * width, (b + 1) * width)
        mine = hot_s[b * n:(b + 1) * n, :].astype(f32)
        wide_offset = jnp.concatenate([offset] * (width // 128), axis=1)
        place_in = (within_s[b * n:(b + 1) * n, :] + wide_offset) * mine
        rank = jnp.sum(place_in, axis=0, keepdims=True).astype(i32)
        rank_s[0:1, spot] = rank
        slot_hot = jnp.where(slot_iota == rank, 1.0, 0.0).astype(bf)
        named = jnp.concatenate([mine * lane_f, mine * float(b)], axis=0).astype(bf)
        inverse = inverse + mm_t(named, slot_hot)
        offset = offset + sums[b * n:(b + 1) * n, :]
    source = (inverse[0:n] + float(width) * inverse[n:2 * n]).astype(i32)
    tile_of, lane_of = source // 128, lax.rem(source, 128)
    found = [jnp.zeros((n, 128), f32) for _ in range(4)]
    for t in range(rows // 128):
        spot = slice(t * 128, (t + 1) * 128)
        here = tile_of == t
        for c in range(4):
            row = coord_ref[c:c + 1, spot] if c < 3 else elem_ref[0:1, spot].astype(f32)
            picked = jnp.take_along_axis(jnp.broadcast_to(row, (n, 128)), lane_of, axis=1)
            found[c] = jnp.where(here, picked, found[c])
    found[3] = found[3] + jnp.where(source < half_rows, float(ez), 0.0)
    for c in range(4):
        for d in range(n):
            asked[d, c:c + 1, :] = found[c][d:d + 1, 0:cap]

    pl.semaphore_wait(barrier, n - 1)

    own_group = me // per

    def ask(a, carry):
        px = lax.rem(gx + nx // 2 + a, nx)
        for b in range(ny):
            @pl.when((px != gx) | (gy != b))
            def _(b=b):
                pltpu.make_async_remote_copy(
                    src_ref=asked.at[px * ny + b], dst_ref=got.at[me],
                    send_sem=ask_send, recv_sem=ask_recv.at[own_group],
                    device_id=(px, b), device_id_type=MESH,
                ).start()

        return carry

    lax.fori_loop(0, nx, ask, 0)

    k_iota = lax.broadcasted_iota(i32, (8, ez), 0)
    e_iota = lax.broadcasted_iota(i32, (8, ez), 1)
    w_k = jnp.zeros((8, ez), f32)
    for k in range(8):
        w_k = jnp.where(k_iota == k, volume_factor * weights[k], w_k)
    joined = ((k_iota == 0) & (e_iota > 0)) | ((k_iota == 7) & (e_iota < ez - 1))
    inv_k = time_step / jnp.where(joined, 2.0 * w_k, w_k)
    inv_x = [1.0 / v for v in weights]
    inv_y = [1.0 / v for v in weights]
    inv_x[0] = jnp.where(gx > 0, 0.5, 1.0) * inv_x[0]
    inv_x[7] = jnp.where(gx < nx - 1, 0.5, 1.0) * inv_x[7]
    inv_y[0] = jnp.where(gy > 0, 0.5, 1.0) * inv_y[0]
    inv_y[7] = jnp.where(gy < ny - 1, 0.5, 1.0) * inv_y[7]
    for i in range(8):
        for j in range(8):
            wm[i, 8 * j:8 * j + 8, :] = (weights[i] * weights[j]) * w_k
            dim[i, 8 * j:8 * j + 8, :] = (inv_x[i] * inv_y[j]) * inv_k

    part = 256
    for m in range(2):
        for b in range(half_rows // part):
            spot = slice(m * half_rows + b * part, m * half_rows + (b + 1) * part)
            to = slice(b * part, (b + 1) * part)
            point = point_ref[0:1, spot]
            eight = lax.broadcasted_iota(i32, (8, part), 0)
            tall = jnp.concatenate([eight + (64 * i + 8 * j) for i, j in FACE + INTERIOR], axis=0)
            short = lax.broadcasted_iota(i32, (ez, part), 0)
            spread_q[m, :, to] = jnp.where(tall == point // ez, 1.0, 0.0).astype(bf)
            spread_e[m, :, to] = jnp.where(short == lax.rem(point, ez), 1.0, 0.0).astype(bf)
        count = mm_t(spread_q[m], spread_e[m])
        for at, (i, j) in enumerate(FACE + INTERIOR):
            spot = slice(8 * j, 8 * j + 8)
            held[m, i, spot] = count[8 * at:8 * at + 8] * (penalty_rate * wm[i, spot])

    for load in loads:
        load.wait()

    def halo_copy(s, m, number):
        dx, dy = HEADINGS[number]
        lines = pl.ds(0 if dy < 0 else 56, 8)
        plane = 0 if dx < 0 else 7
        if dy == 0:
            source, target = local.at[m, plane], hx.at[s, number, m]
        elif dx == 0:
            source, target = local.at[m, :, lines, :], hy.at[s, number - 2, m]
        else:
            source, target = local.at[m, plane, lines, :], he.at[s, number - 4, m]
        return pltpu.make_async_remote_copy(
            src_ref=source, dst_ref=target, send_sem=halo_send.at[s, m, number], recv_sem=halo_recv.at[s, m, number],
            device_id=(gx + dx, gy + dy), device_id_type=MESH,
        )

    def inside(dx, dy):
        return (gx + dx >= 0) & (gx + dx < nx) & (gy + dy >= 0) & (gy + dy < ny)

    def operators(value):
        for m in range(2):
            lo = slice(m * ez, (m + 1) * ez)
            scale = nu_ref[m:m + 1, :]
            for half in range(2):
                some = slice(4 * half, 4 * half + 4)
                part = value[m, some].reshape(256, ez)
                grad[0, some, :, lo] = mm3(ops[0], ops[1], part).reshape(4, 64, ez)
                grad[1, some, :, lo] = mm3(ops[2], ops[3], part).reshape(4, 64, ez)
            for a in range(8):
                gxa = (2.0 * derivative[a][0]) * value[m, 0]
                for i in range(1, 8):
                    gxa = gxa + (2.0 * derivative[a][i]) * value[m, i]
                wma = wm[a]
                gya = grad[0, a, :, lo]
                gza = grad[1, a, :, lo]
                adv = vel[0, m, a] * gxa + vel[1, m, a] * gya + vel[2, m, a] * gza
                local[m, a] = -(wma * adv) - held[m, a] * value[m, a]
                wn = wma * scale
                work[m, a] = wn * gxa
                grad[0, a, :, lo] = wn * gya
                grad[1, a, :, lo] = wn * gza
            for half in range(2):
                some = slice(4 * half, 4 * half + 4)
                part_y = grad[0, some, :, lo].reshape(256, ez)
                part_z = grad[1, some, :, lo].reshape(256, ez)
                back = mm3(ops[4], ops[5], part_y) + mm3(ops[6], ops[7], part_z)
                local[m, some] -= back.reshape(4, 64, ez)
            for i in range(8):
                total = (2.0 * derivative[0][i]) * work[m, 0]
                for a in range(1, 8):
                    total = total + (2.0 * derivative[a][i]) * work[m, a]
                local[m, i] -= total

    operators(start)
    pltpu.make_async_copy(asked.at[me], got.at[me], in_sem.at[0]).start()
    pltpu.make_async_copy(asked.at[me], got.at[me], in_sem.at[0]).wait()
    def prepare(g):
        wanted = jnp.concatenate([got[g * per + t] for t in range(per)], axis=1)
        wide = lax.broadcasted_iota(i32, (2 * ez, lanes), 0)
        pick[g] = jnp.where(wide == wanted[3:4].astype(i32), 1.0, 0.0).astype(bf)
        away = [wanted - v for v in gll_nodes]
        before = [None, away[0]]
        for k in range(1, 7):
            before.append(before[-1] * away[k])
        after = [None] * 7 + [None]
        after[6] = away[7]
        for k in range(5, -1, -1):
            after[k] = after[k + 1] * away[k + 1]
        for j in range(8):
            norm = 1.0
            for k in range(8):
                if k != j:
                    norm *= gll_nodes[j] - gll_nodes[k]
            factor = after[0] if j == 0 else before[7] if j == 7 else before[j] * after[j]
            factor = factor * (1.0 / norm)
            for c in range(3):
                basis_ref[g, 8 * c + j:8 * c + j + 1, :] = factor[c:c + 1]

    def split_lines(value, lines, into):
        both = jnp.concatenate(
            [jnp.concatenate([value[m, i, 8 * j:8 * j + 8] for i, j in lines], axis=0) for m in range(2)], axis=1
        )
        lhs[0, into, :], lhs[1, into, :] = halves(both)

    face_at, inner_at = slice(0, 8 * len(FACE)), slice(8 * len(FACE), 512)

    def contract(lines, at_rows, g):
        found = mm(lhs[0, at_rows], pick[g]) + mm(lhs[1, at_rows], pick[g])
        total = None
        for j in range(8):
            line = None
            for at, (i, jj) in enumerate(lines):
                if jj == j:
                    term = found[8 * at:8 * at + 8] * basis_ref[g, i:i + 1, :]
                    line = term if line is None else line + term
            if line is not None:
                line = line * basis_ref[g, 8 + j:9 + j, :]
                total = line if total is None else total + line
        return total

    def sum_third(flat, m, first, size, stride):
        lane = lax.broadcasted_iota(i32, (size, ez), 1)
        low_rows, high_rows = pl.ds(first, size, stride=stride), pl.ds(first + 7, size, stride=stride)
        lower, upper = flat[m, low_rows, :], flat[m, high_rows, :]
        shared = upper + pltpu.roll(lower, ez - 1, 1)
        flat[m, high_rows, :] = jnp.where(lane < ez - 1, shared, upper)
        flat[m, low_rows, :] = jnp.where(lane > 0, pltpu.roll(shared, 1, 1), lower)

    flat = local.reshape(2, 512, ez)

    def halo_sent(s):
        for m in range(2):
            for number, (dx, dy) in enumerate(HEADINGS):
                @pl.when(inside(dx, dy))
                def _(m=m, number=number):
                    halo_copy(s, m, number).wait_send()

    for s in range(3):
        value = start if s == 0 else cur
        split_lines(value, FACE, face_at)

        def interpolate(g):
            if s == 0:
                total = contract(FACE + INTERIOR, slice(0, 512), g)
            else:
                total = contract(FACE, face_at, g) + inner_part[g]
            row = jnp.sum(total * basis_ref[g, 16:24, :], axis=0, keepdims=True)
            for t in range(per):
                ans[s, g * per + t] = row[:, t * cap:(t + 1) * cap]
            for t in range(per):
                d = g * per + t

                @pl.when(d != me)
                def _(d=d):
                    pltpu.make_async_remote_copy(
                        src_ref=ans.at[s, d], dst_ref=rep.at[s, me],
                        send_sem=ans_send.at[s], recv_sem=ans_recv.at[s],
                        device_id=place(d), device_id_type=MESH,
                    ).start()

        def from_afar(p, carry):
            off = groups // 2 + ((p + 1) // 2) * (1 - 2 * lax.rem(p, 2))
            interpolate(lax.rem(own_group + off + groups, groups))
            return carry

        def request(p, carry):
            off = ((p + 1) // 2) * (1 - 2 * lax.rem(p, 2))
            g = lax.rem(own_group + off + groups, groups)
            some = got.at[pl.ds(0, per)]
            pltpu.make_async_copy(some, some, ask_recv.at[g]).wait()
            prepare(g)
            return carry

        if s == 0:
            split_lines(value, INTERIOR, inner_at)
            nearby = got.at[pl.ds(0, per - 1)]
            pltpu.make_async_copy(nearby, nearby, ask_recv.at[own_group]).wait()
            prepare(own_group)
            early = 2

            def soon(p, carry):
                interpolate(lax.rem(own_group - p + groups, groups))
                return carry

            if early > 1:
                lax.fori_loop(1, early, request, 0)
            lax.fori_loop(0, early, soon, 0)
            lax.fori_loop(max(early, 1), groups, request, 0)
            lax.fori_loop(0, groups - early, from_afar, 0, unroll=2)
        else:
            lax.fori_loop(0, groups, from_afar, 0, unroll=2)
            halo_sent(s - 1)
        if s > 0:
            operators(cur)
        rep[s, me] = ans[s, me]
        arrived = ans.at[s, pl.ds(0, n - 1)]
        pltpu.make_async_copy(arrived, arrived, ans_recv.at[s]).wait()

        answers = jnp.concatenate([rep[s, d] for d in range(n)], axis=0)
        if cap < 128:
            answers = jnp.concatenate([answers, jnp.zeros((n, 128 - cap), f32)], axis=1)

        def scatter(m, lines, first):
            added = mm_t(spread_q[m, first:first + 8 * len(lines), :], spread_v[m])
            for at, (i, j) in enumerate(lines):
                spot, rows_at = slice(8 * j, 8 * j + 8), slice(8 * at, 8 * at + 8)
                local[m, i, spot] += (penalty_rate * wm[i, spot]) * (added[rows_at, :ez] + added[rows_at, ez:])

        spread_v = []
        for m in range(2):
            pieces = []
            for t in range(half_rows // 128):
                spot = slice(m * half_rows + t * 128, m * half_rows + (t + 1) * 128)
                slot = jnp.broadcast_to(rank_s[0:1, spot], (n, 128))
                taken = jnp.take_along_axis(answers, slot, axis=1)
                own = owner_ref[0:1, spot] == lax.broadcasted_iota(i32, (n, 128), 0)
                pieces.append(jnp.sum(jnp.where(own, taken, 0.0), axis=0, keepdims=True))
            row_high, row_low = halves(jnp.concatenate(pieces, axis=1))
            where_e = spread_e[m]
            spread_v.append(jnp.concatenate([where_e * row_high, where_e * row_low], axis=0))
            scatter(m, FACE, 0)
            for i in (0, 7):
                sum_third(flat, m, 64 * i + 8, 6, 8)
            for j in (0, 7):
                sum_third(flat, m, 8 * j, 8, 64)
            for number, (dx, dy) in enumerate(HEADINGS):
                @pl.when(inside(dx, dy))
                def _(m=m, number=number):
                    halo_copy(s, m, number).start()

        target = cur if s < 2 else out_ref
        share = (1.0, 0.25, 2.0 / 3.0)[s]
        for m in range(2):
            scatter(m, INTERIOR, 8 * len(FACE))
            for i in INNER:
                sum_third(flat, m, 64 * i + 8, 6, 8)
            for i in range(8):
                moved = value[m, i] + local[m, i] * dim[i]
                if s == 0:
                    cur[m, i] = moved
                elif s == 1:
                    cur[m, i] = 0.75 * start[m, i] + 0.25 * moved
                else:
                    out_ref[m, i] = start[m, i] * (1.0 / 3.0) + (2.0 / 3.0) * moved
        if s < 2:
            split_lines(cur, INTERIOR, inner_at)

            def ahead(g, carry):
                inner_part[g] = contract(INTERIOR, inner_at, g)
                return carry

            lax.fori_loop(0, groups, ahead, 0, unroll=2)
        for m in range(2):
            for number, (dx, dy) in enumerate(HEADINGS):
                @pl.when(inside(-dx, -dy))
                def _(m=m, number=number, dx=dx, dy=dy):
                    halo_copy(s, m, number).wait_recv()
                    plane = 7 if dx < 0 else 0
                    lines = slice(56, 64) if dy < 0 else slice(0, 8)
                    if dy == 0:
                        target[m, plane] += hx[s, number, m] * (share * dim[plane])
                    elif dx == 0:
                        target[m, :, lines, :] += hy[s, number - 2, m] * (share * dim[:, lines, :])
                    else:
                        target[m, plane, lines, :] += he[s, number - 4, m] * (share * dim[plane, lines, :])
    halo_sent(2)
    sent = got.at[pl.ds(0, n - 1)]
    pltpu.make_async_copy(sent, sent, ask_send).wait()
    for s in range(3):
        whole = ans.at[s, pl.ds(0, n - 1)]
        pltpu.make_async_copy(whole, whole, ans_send.at[s]).wait()


def split_host(matrix):
    high = matrix.astype(jnp.bfloat16)
    low = (matrix - high.astype(np.float64)).astype(jnp.bfloat16)
    return [high, low]


def body(scalar, velocity, diffusivity, recv_owner, donor_elem, recv_point, recv_coords):
    tables = gll_tables()
    derivative = tables[2]
    ez = scalar.shape[4]
    n = lax.axis_size("gx") * lax.axis_size("gy")
    rows = recv_owner.shape[0]
    cap = max(2, 2 * rows // n)
    per = max(1, min(n, 512 // cap))
    groups, lanes = n // per, per * cap
    width = min(256, rows)
    blocks = rows // width
    bf, f32, i32 = jnp.bfloat16, jnp.float32, jnp.int32

    half_eye = np.eye(4)
    table = 2.0 * np.asarray(derivative, np.float64)
    along_y = np.kron(half_eye, np.kron(table, np.eye(8)))
    along_z = np.kron(half_eye, np.kron(np.eye(8), table))
    ops = []
    for matrix in (along_y, along_z, along_y.T, along_z.T):
        ops = ops + split_host(matrix)
    ops = jnp.asarray(np.stack(ops))

    vmem = pltpu.VMEM
    dma = pltpu.SemaphoreType.DMA
    field = (2, 8, 64, ez)
    in_vmem, anywhere = pl.BlockSpec(memory_space=vmem), pl.BlockSpec(memory_space=pltpu.HBM)
    out = pl.pallas_call(
        functools.partial(step_kernel, tables),
        out_shape=jax.ShapeDtypeStruct(field, f32),
        in_specs=[in_vmem] * 5 + [anywhere] * 3,
        out_specs=in_vmem,
        scratch_shapes=[
            vmem(field, f32),
            vmem((3,) + field, f32),
            vmem((8, 256, 256), bf),
            vmem(field, f32),
            vmem(field, f32),
            vmem(field, f32),
            vmem((2, 8, 64, 2 * ez), f32),
            vmem((8, 64, ez), f32),
            vmem((8, 64, ez), f32),
            vmem(field, f32),
            vmem((blocks * n, width), bf),
            vmem((blocks * n, width), f32),
            vmem((1, rows), i32),
            vmem((n, 4, cap), f32),
            vmem((n, 4, cap), f32),
            vmem((groups, 2 * ez, lanes), bf),
            vmem((groups, 24, lanes), f32),
            vmem((2, 512, rows // 2), bf),
            vmem((2, ez, rows // 2), bf),
            vmem((3, n, 1, cap), f32),
            vmem((3, n, 1, cap), f32),
            vmem((3, 2, 2, 64, ez), f32),
            vmem((3, 2, 2, 8, 8, ez), f32),
            vmem((3, 4, 2, 8, ez), f32),
            vmem((2, 512, 2 * ez), bf),
            vmem((groups, 8, lanes), f32),
            dma((3,)),
            dma,
            dma((groups,)),
            dma((3,)),
            dma((3,)),
            dma((3, 2, 8)),
            dma((3, 2, 8)),
        ],
        compiler_params=pltpu.CompilerParams(collective_id=0, has_side_effects=True, vmem_limit_bytes=44 * 1024 * 1024),
        name="advance",
    )(
        *[pltpu.with_memory_space_constraint(v, pltpu.HBM) for v in (
            recv_owner.reshape(1, rows), donor_elem.reshape(1, rows), recv_point.reshape(1, rows), recv_coords,
            diffusivity.reshape(2, ez), scalar.reshape(field), velocity.reshape((3,) + field), ops,
        )]
    )
    return out.reshape(scalar.shape)


def solution(mesh):
    return jax.shard_map(
        body,
        mesh=mesh,
        in_specs=(
            P(None, None, "gx", "gy", None),
            P(None, None, None, "gx", "gy", None),
            P(None, "gx", "gy", None),
            P(("gx", "gy"), None),
            P(("gx", "gy")),
            P(("gx", "gy")),
            P(None, ("gx", "gy")),
        ),
        out_specs=P(None, None, "gx", "gy", None),
        check_vma=False,
    )
```
